128 devices in a mesh: mem: 8 (over x_hi, y), lat: 16 (over x_lo, z, core).
Axes of the slice: x: 4 (x_hi: 2, x_lo: 2; x = x_hi * 2 + x_lo), y: 4, z: 4, core: 2. Of those that a mesh axis runs over, the one named last changes fastest.
Arguments:
- controls: float32 [48, 16, 16, 96], P('mem', None, 'lat'), may hold values from -6 to 6
- perturbations: bfloat16 [48, 64, 64, 384], P('mem', None, 'lat'), may hold values from -0.875 to 0.875
- precision_weight: bfloat16 [64, 256, 1536], P(None, 'lat'), may hold values from 0.25 to 4
- north_coef: float32 [256, 1536], P('lat'), may hold values from 0.02 to 0.24
- east_coef: float32 [256, 1536], P('lat'), may hold values from 0.02 to 0.24
- fine_source: int32 [256], P('lat'), may hold values from 0 to 62, as said below
- fine_frac: float32 [256], P('lat'), may hold values from 0 to 1
Outputs:
- gradient: float32 [48, 16, 16, 96], P('mem', None, 'lat')
The draws below stay inside these ranges and needn't reach their ends.
Inputs may be any that keep to these rules, and one draw needn't show every extreme that they name: Fine row f lies in band b = f // 16; its source rows fine_source[f] and fine_source[f] + 1 satisfy max(b * 4 - 4, 0) <= fine_source[f] <= min((b + 1) * 4 + 2, 62), and both ends are reached in every band.
All inputs are finite; a program needn't handle non-finite values.
Results may differ from the reference program's by a relative error of at most 0.0003.
Values sent between devices are 32-bit elements; how exact they have to be, the bound alone decides.
No kernel may reach another device: no remote copies, remote signals or barrier semaphores. Data moves between devices by JAX's collectives and lax.ppermute only.
A program may use at most 128 MiB of HBM per device.

```python
import math
import jax
import jax.numpy as jnp
from jax import lax

CLEV = 16
CLON = 96
PASSES = 5
REACH = 4
MEMBERS = 48
LEV = 64
CLAT = 16
MROWS = 4
FROWS = 16
MLAT = 64
FLAT = 256
MLON = 384
FLON = 1536


def draw_fine_source(key, part):
    rows_all = jnp.arange(FLAT, dtype=jnp.int32)
    band = rows_all // FROWS
    within = rows_all % FROWS
    start = band * MROWS
    lowest = jnp.maximum(start - REACH, 0)
    highest = jnp.minimum(start + MROWS + REACH - 2, MLAT - 2)
    base = start + within * MROWS // FROWS
    jitter = jax.random.randint(key, (FLAT,), -REACH, REACH + 1, dtype=jnp.int32)
    source = jnp.clip(base + jitter, lowest, highest)
    source = jnp.where(within == 0, lowest, source)
    source = jnp.where(within == FROWS - 1, highest, source)
    return source.astype(jnp.int32)


def steps_of(own_key, extent, cuts, smallest, largest):
    def one(dim, blocks):
        draws = jax.random.uniform(jax.random.fold_in(jax.random.fold_in(own_key, 6), dim), (blocks,), jnp.float32, smallest / len(cuts), largest / len(cuts))
        return jnp.repeat(jnp.exp(draws), extent[dim] // blocks).reshape((-1,) + (1,) * (len(extent) - dim - 1))

    level = one(*cuts[0])
    for cut in cuts[1:]:
        level = level * one(*cut)
    return level


def centred(key, extent, width, limit, pieces=(), kind=jnp.bfloat16):
    gain = steps_of(key, extent, pieces, -0.22, 0.18) if pieces else 1.0
    values = jax.random.normal(key, extent, jnp.float32) * width * gain
    return jnp.minimum(jnp.maximum(values, -limit), limit).astype(kind)


def setup_inputs(seed: int = 0) -> dict:
    splits = jax.random.split(jax.random.key(seed), 8)
    controls = centred(splits[0], (MEMBERS, CLEV, CLAT, CLON), 1.0, 6.0, ((0, 8), (2, 16)), jnp.float32)
    perturbations = centred(splits[1], (MEMBERS, LEV, MLAT, MLON), MEMBERS ** -0.5, 0.875, ((0, 8), (2, 16)))
    precision_weight = jnp.clip(jnp.exp(math.log(4.0) - 2.7725887 * jax.random.uniform(splits[2], (LEV, FLAT, FLON), jnp.float32) ** steps_of(splits[2], (LEV, FLAT, FLON), ((1, 16),), -0.2, 0.2)), 0.25, 4.0).astype(jnp.bfloat16)
    north_coef = jnp.clip(0.02 + 0.22 * jax.random.uniform(splits[3], (FLAT, FLON), jnp.float32) ** steps_of(splits[3], (FLAT, FLON), ((0, 16),), -0.2, 0.2), 0.02, 0.24)
    east_coef = jnp.clip(0.02 + 0.22 * jax.random.uniform(splits[4], (FLAT, FLON), jnp.float32) ** steps_of(splits[4], (FLAT, FLON), ((0, 16),), -0.2, 0.2), 0.02, 0.24)
    fine_source = draw_fine_source(jax.random.fold_in(splits[7], 71), 0)
    fine_frac = jnp.clip(1.0 * jax.random.uniform(splits[6], (FLAT,), jnp.float32) ** steps_of(splits[6], (FLAT,), ((0, 16),), -0.2, 0.2), 0.0, 1.0)
    return dict(controls=controls, perturbations=perturbations, precision_weight=precision_weight, north_coef=north_coef, east_coef=east_coef, fine_source=fine_source, fine_frac=fine_frac)


def refine(padded, dimension):
    count = padded.shape[dimension] - 2
    previous = lax.slice_in_dim(padded, 0, count, axis=dimension)
    current = lax.slice_in_dim(padded, 1, count + 1, axis=dimension)
    following = lax.slice_in_dim(padded, 2, count + 2, axis=dimension)
    phases = [0.375 * previous + 0.625 * current, 0.125 * previous + 0.875 * current, 0.875 * current + 0.125 * following, 0.625 * current + 0.375 * following]
    stacked = jnp.stack(phases, axis=dimension + 1)
    new_shape = list(padded.shape)
    new_shape[dimension] = 4 * count
    return stacked.reshape(new_shape)

def raise_padded(padded):
    field = refine(jnp.pad(padded, ((0, 0), (1, 1), (0, 0), (0, 0)), mode='edge'), 1)
    field = refine(jnp.pad(field, ((0, 0), (0, 0), (0, 0), (1, 1)), mode='wrap'), 3)
    return refine(field, 2)

def diffuse(padded, north_pad, east_rows):
    center = padded[:, 1:-1]
    upward = north_pad[1:-1] * (padded[:, 2:] - center)
    downward = north_pad[:-2] * (padded[:, :-2] - center)
    eastward = east_rows * (jnp.roll(center, -1, 2) - center)
    westward = jnp.roll(east_rows, 1, 1) * (jnp.roll(center, 1, 2) - center)
    return center + upward + downward + eastward + westward

def to_fine(increment, fine_source, fine_frac):
    lower_rows = jnp.take(increment, fine_source, axis=1)
    upper_rows = jnp.take(increment, fine_source + 1, axis=1)
    fraction = fine_frac[:, None]
    blended = (1.0 - fraction) * lower_rows + fraction * upper_rows
    return refine(jnp.pad(blended, ((0, 0), (0, 0), (1, 1)), mode='wrap'), 2)

def reference(controls, perturbations, precision_weight, north_coef, east_coef, fine_source, fine_frac):

    def raise_one(member_control):
        padded = jnp.pad(member_control[None], ((0, 0), (0, 0), (1, 1), (0, 0)), mode='edge')
        return raise_padded(padded)[0]

    def accumulate(running, member_pair):
        return (running + member_pair[1].astype(jnp.float32) * raise_one(member_pair[0]), None)
    start_sum = jnp.zeros((LEV, MLAT, MLON), jnp.float32)
    increment, _ = lax.scan(accumulate, start_sum, (controls, perturbations))
    fine_grid, pull_fine = jax.vjp(lambda field: to_fine(field, fine_source, fine_frac), increment)
    zero_row = jnp.zeros((1, FLON), jnp.float32)
    north_pad = jnp.concatenate([zero_row, north_coef, zero_row], axis=0)

    def smooth(field):
        for repeat in range(PASSES):
            field = diffuse(jnp.pad(field, ((0, 0), (1, 1), (0, 0))), north_pad, east_coef)
        return field
    weighted = precision_weight.astype(jnp.float32) * smooth(fine_grid)
    fine_adjoint = pull_fine(smooth(weighted))[0]

    def adjoint_one(member_pair):
        _, pull_back = jax.vjp(raise_one, member_pair[0])
        return pull_back(member_pair[1].astype(jnp.float32) * fine_adjoint)[0]
    adjoints = lax.map(adjoint_one, (controls, perturbations))
    return controls + adjoints
```

```python
import jax
import jax.numpy as jnp
import numpy as np
from jax import lax
from jax.experimental import pallas as pl
from jax.experimental.pallas import tpu as pltpu
from jax.sharding import PartitionSpec as P

PASSES = 5
REACH = 4
HALO = 2 * PASSES
F32 = jnp.float32
BF16 = jnp.bfloat16

PHASES = np.array(
    [[0.375, 0.625, 0.0], [0.125, 0.875, 0.0], [0.0, 0.875, 0.125], [0.0, 0.625, 0.375]]
)


def refine_matrix(count, periodic):
    matrix = np.zeros((4 * count, count), np.float32)
    for q in range(count):
        for r in range(4):
            for step in range(3):
                source = q + step - 1
                source = source % count if periodic else min(max(source, 0), count - 1)
                matrix[4 * q + r, source] += PHASES[r, step]
    return matrix


def split2(x):
    hi = x.astype(BF16)
    lo = (x - hi.astype(F32)).astype(BF16)
    return hi, lo


def dot(a, b):
    return jnp.dot(a, b, preferred_element_type=F32)


def prepare_kernel(place, weight, north, east, extra, select, order, coef, own_weight, buf_a, buf_b):
    odd = place[0] % 2
    levels, rows, lon = weight.shape
    stacked = jnp.concatenate([north[...], east[...]], axis=0)
    hi, rest = stacked.astype(BF16), None
    rest = stacked - hi.astype(F32)
    mid = rest.astype(BF16)
    low = (rest - mid.astype(F32)).astype(BF16)
    sel = select[...]
    values = dot(order[...], weight[...].reshape(levels * rows, lon)).astype(BF16)
    quarter = lon // 4
    for c in range(lon // 512):
        cut = slice(512 * c, 512 * c + 512)
        cpart = dot(hi[:, cut], sel) + dot(mid[:, cut], sel) + dot(low[:, cut], sel)
        wpart = dot(values[:, cut], sel)
        for r in range(4):
            to = slice(quarter * r + 128 * c, quarter * r + 128 * c + 128)
            frm = slice(128 * r, 128 * r + 128)
            coef[:, to] = cpart[:, frm]
            own_weight[:, :, to] = wpart[:, frm].reshape(rows, levels, 128)

    def fill(buf, upper):
        first = rows - PASSES if upper else 0
        for k in range(PASSES):
            buf[8 * k : 8 * k + 8, :] = own_weight[first + k]
        first = rows - HALO if upper else 0
        base = 8 * PASSES
        buf[base : base + HALO, :] = coef[first : first + HALO, :]
        buf[base + HALO : base + 2 * HALO, :] = coef[rows + first : rows + first + HALO, :]
        buf[base + 2 * HALO :, :] = extra[...]

    @pl.when(odd == 0)
    def _():
        fill(buf_a, True)
        fill(buf_b, False)

    @pl.when(odd == 1)
    def _():
        fill(buf_a, False)
        fill(buf_b, True)


def assemble_kernel(place, coef, own_weight, got_a, got_b, north, east, west, weight):
    lat = place[0]
    odd = lat % 2
    rows = own_weight.shape[0]
    quarter = coef.shape[1] // 4

    def put(i, nrow, erow):
        shape = (8, coef.shape[1])
        north[i] = jnp.broadcast_to(nrow, shape)
        spread = jnp.broadcast_to(erow, shape)
        east[i] = spread
        west[i] = pltpu.roll(spread[:, 3 * quarter :], 1, axis=1)

    for k in range(rows):
        put(HALO + k, coef[k : k + 1, :], coef[rows + k : rows + k + 1, :])
        weight[PASSES + k] = own_weight[k]

    def side(buf, start, wstart):
        base = 8 * PASSES
        for k in range(HALO):
            put(start + k, buf[base + k : base + k + 1, :], buf[base + HALO + k : base + HALO + k + 1, :])
        for k in range(PASSES):
            weight[wstart + k] = buf[8 * k : 8 * k + 8, :]

    @pl.when(odd == 0)
    def _():
        side(got_b, 0, 0)
        side(got_a, HALO + rows, PASSES + rows)

    @pl.when(odd == 1)
    def _():
        side(got_a, 0, 0)
        side(got_b, HALO + rows, PASSES + rows)

    @pl.when(lat == 0)
    def _():
        north[HALO - 1] = jnp.zeros(north.shape[1:], F32)


def raise_kernel(place, own, got_a, got_b, pert, lon_up, mix, out, x, acc):
    lat, last = place[0], place[1] - 1
    odd = lat % 2
    members = pert.shape[0]
    lev = own.shape[0] // members

    def put(step, ref):
        for m in range(members):
            at = (3 * m + step) * lev
            x[at : at + lev, :] = ref[m * lev : m * lev + lev, :]

    put(1, own)

    @pl.when(lat == 0)
    def _():
        put(0, own)

    @pl.when((lat > 0) & (odd == 0))
    def _():
        put(0, got_b)

    @pl.when(odd == 1)
    def _():
        put(0, got_a)

    @pl.when(lat == last)
    def _():
        put(2, own)

    @pl.when((lat < last) & (odd == 1))
    def _():
        put(2, got_b)

    @pl.when(odd == 0)
    def _():
        put(2, got_a)

    hi, lo = split2(x[...])
    wide = dot(hi, lon_up[...]) + dot(lo, lon_up[...])
    for m in range(members):
        hi, lo = split2(wide[3 * lev * m : 3 * lev * (m + 1), :])
        field = dot(mix[...], jnp.concatenate([hi, lo], axis=0))
        term = field * pert[m].astype(F32)
        if m == 0:
            acc[...] = term
        elif m < members - 1:
            acc[...] += term
        else:
            out[...] = (acc[...] + term).reshape(out.shape)


def total_kernel(parts, out, sums):
    count, n, lon = parts.shape
    total = parts[0]
    for k in range(1, count):
        total = total + parts[k]
    rows = n // 8
    for c in range(lon // 128):
        lanes = slice(128 * c, 128 * c + 128)
        sums[n * c : n * c + n, :] = total[:, lanes]
        for row in range(rows):
            out[8 * row : 8 * row + 8, lanes] = sums[pl.ds(n * c + row, 8, stride=rows), :]


def fine_kernel(
    place, source, frac, extra_a, extra_b, own, mate, up_pair, down_pair,
    north, east, west, weight, keep, send_a, send_b, mid, v, acc,
):
    lat, last = place[0], place[1] - 1
    odd = lat % 2
    lon = own.shape[1]
    rows = source.shape[0]
    n = rows + 2 * HALO
    band = own.shape[0] // 8

    def bring(slot, ref, start):
        for k in range(band):
            mid[slot * band + k] = ref[start + 8 * k : start + 8 * k + 8, :]

    half = own.shape[0]
    bring(2, own, 0)

    @pl.when(odd == 0)
    def _():
        bring(0, up_pair, 0)
        bring(1, up_pair, half)
        bring(3, mate, 0)
        bring(4, down_pair, 0)

    @pl.when(odd == 1)
    def _():
        bring(0, up_pair, 0)
        bring(1, mate, 0)
        bring(3, down_pair, half)
        bring(4, down_pair, 0)

    origin = (lat - 2) * band
    for i in range(n):
        k = i - HALO
        if k < 0:
            k += rows
            f = jnp.where(odd == 1, extra_a[0, k], extra_b[0, k])
            s = jnp.where(odd == 1, extra_a[0, rows + k], extra_b[0, rows + k]).astype(jnp.int32)
            valid = jnp.where(lat > 0, 1.0, 0.0)
        elif k >= rows:
            k -= rows
            f = jnp.where(odd == 0, extra_a[0, k], extra_b[0, k])
            s = jnp.where(odd == 0, extra_a[0, rows + k], extra_b[0, rows + k]).astype(jnp.int32)
            valid = jnp.where(lat < last, 1.0, 0.0)
        else:
            f, s, valid = frac[k], source[k], None
        s = jnp.clip(s - origin, 0, 5 * band - 2)
        below, above = 1.0 - f, f
        if valid is not None:
            below, above = below * valid, above * valid
        cur = below * mid[s] + above * mid[s + 1]
        prev = pltpu.roll(cur, 1, axis=1)
        nxt = pltpu.roll(cur, lon - 1, axis=1)
        v[i, :, 0:lon] = 0.375 * prev + 0.625 * cur
        v[i, :, lon : 2 * lon] = 0.125 * prev + 0.875 * cur
        v[i, :, 2 * lon : 3 * lon] = 0.875 * cur + 0.125 * nxt
        v[i, :, 3 * lon : 4 * lon] = 0.625 * cur + 0.375 * nxt

    inside_top = jnp.where(lat < last, 1.0, 0.0)

    def cut(r):
        return slice(r * lon, r * lon + lon)

    def sweep(first, stop):
        def flux(i, here, there):
            return [north[i, :, cut(r)] * (there[r] - here[r]) for r in range(4)]

        before = [v[first - 1, :, cut(r)] for r in range(4)]
        here = [v[first, :, cut(r)] for r in range(4)]
        low = flux(first - 1, before, here)
        for i in range(first, stop):
            there = [v[i + 1, :, cut(r)] for r in range(4)]
            high = flux(i, here, there)
            if i == HALO + rows:
                low = [inside_top * x for x in low]
            right = pltpu.roll(here[0], lon - 1, axis=1)
            left = pltpu.roll(here[3], 1, axis=1)
            side = [
                east[i, :, cut(r)] * ((here[r + 1] if r < 3 else right) - here[r]) for r in range(4)
            ]
            back = [west[i] * (here[0] - left)] + side[:3]
            for r in range(4):
                v[i, :, cut(r)] = here[r] + ((high[r] - low[r]) + (side[r] - back[r]))
            low, here = high, there

    def first_pass(_, carry):
        sweep(1, n - 1)
        return carry

    lax.fori_loop(0, PASSES, first_pass, 0)

    def scale(k, carry):
        v[PASSES + k] = weight[k] * v[PASSES + k]
        return carry

    lax.fori_loop(0, rows + 2 * PASSES, scale, 0)

    def second_pass(_, carry):
        sweep(PASSES + 1, n - PASSES - 1)
        return carry

    lax.fori_loop(0, PASSES, second_pass, 0)

    acc[...] = jnp.zeros(acc.shape, F32)
    base = (lat - 1) * band
    for k in range(rows):
        o = [v[HALO + k, :, cut(r)] for r in range(4)]
        ahead = pltpu.roll(0.375 * o[0] + 0.125 * o[1], lon - 1, axis=1)
        behind = pltpu.roll(0.125 * o[2] + 0.375 * o[3], 1, axis=1)
        g = 0.625 * (o[0] + o[3]) + 0.875 * (o[1] + o[2]) + (ahead + behind)
        s = jnp.clip(source[k] - base, 0, 3 * band - 2)
        f = frac[k]
        acc[s] += (1.0 - f) * g
        acc[s + 1] += f * g
    for k in range(band):
        keep[8 * k : 8 * k + 8, :] = acc[band + k]

    def give(ref, slot):
        for k in range(band):
            ref[8 * k : 8 * k + 8, :] = acc[slot * band + k]

    @pl.when(odd == 0)
    def _():
        give(send_a, 2)
        give(send_b, 0)

    @pl.when(odd == 1)
    def _():
        give(send_a, 0)
        give(send_b, 2)


def copies_kernel(keep, got_a, got_b, out, sums):
    count, n, lon = out.shape
    rows = n // 8
    total = keep[...] + got_a[...] + got_b[...]
    for c in range(lon // 128):
        lanes = slice(128 * c, 128 * c + 128)
        for row in range(rows):
            sums[pl.ds(n * c + row, 8, stride=rows), :] = total[8 * row : 8 * row + 8, lanes]
        value = sums[n * c : n * c + n, :]
        for k in range(count):
            out[k, :, lanes] = value


def lower_kernel(place, pert, adjoint, mix_t, lon_down, own, send_a, send_b, wide):
    lat, last = place[0], place[1] - 1
    odd = lat % 2
    members = pert.shape[0]
    lev = own.shape[0] // members
    field = adjoint[...].reshape(pert.shape[1], pert.shape[2])
    for m in range(members):
        hi, lo = split2(field * pert[m].astype(F32))
        wide[3 * lev * m : 3 * lev * (m + 1), :] = dot(mix_t[...], hi) + dot(mix_t[...], lo)
    hi, lo = split2(wide[...])
    narrow = dot(hi, lon_down[...]) + dot(lo, lon_down[...])
    at_first = jnp.where(lat == 0, 1.0, 0.0)
    at_last = jnp.where(lat == last, 1.0, 0.0)
    is_odd = jnp.where(odd == 1, 1.0, 0.0)
    for m in range(members):
        at = 3 * lev * m
        low = narrow[at : at + lev]
        mine = narrow[at + lev : at + 2 * lev]
        high = narrow[at + 2 * lev : at + 3 * lev]
        to = slice(m * lev, m * lev + lev)
        own[to, :] = mine + at_first * low + at_last * high
        low = (1.0 - at_first) * low
        high = (1.0 - at_last) * high
        send_a[to, :] = is_odd * low + (1.0 - is_odd) * high
        send_b[to, :] = is_odd * high + (1.0 - is_odd) * low


def vmem():
    return pl.BlockSpec(memory_space=pltpu.VMEM)


def smem():
    return pl.BlockSpec(memory_space=pltpu.SMEM)


def call(kernel, name, outs, scratch, scalars, vectors):
    many = isinstance(outs, list)
    shapes = [jax.ShapeDtypeStruct(s, F32) for s in (outs if many else [outs])]
    return pl.pallas_call(
        kernel,
        name=name,
        out_shape=shapes if many else shapes[0],
        in_specs=[smem()] * len(scalars) + [vmem()] * len(vectors),
        out_specs=[vmem()] * len(shapes) if many else vmem(),
        scratch_shapes=[pltpu.VMEM(s, F32) for s in scratch],
        compiler_params=pltpu.CompilerParams(vmem_limit_bytes=48 * 2**20),
    )(*scalars, *vectors)


def body(controls, perturbations, precision_weight, north_coef, east_coef, fine_source, fine_frac):
    lat = lax.axis_index("lat")
    count = lax.axis_size("lat")
    mem = lax.axis_index("mem")
    ranks = lax.axis_size("mem")
    members, clev, _, clon = controls.shape
    lev, band, lon = perturbations.shape[1:]
    rows, fine_lon = north_coef.shape
    part = lev // ranks

    mates = [(i, i ^ 1) for i in range(count)]
    across = [(i, (i + 1) % count if i % 2 else (i - 1) % count) for i in range(count)]
    up_two = [(i, (i + 2) % count) for i in range(count)]
    down_two = [(i, (i - 2) % count) for i in range(count)]

    place = jnp.stack([lat, jnp.int32(count), mem]).astype(jnp.int32)
    lon_refine = refine_matrix(clon, True)
    lev_refine = refine_matrix(clev, False)
    mix = np.einsum("vl,rt->vrtl", lev_refine, PHASES).reshape(lev * band, 3 * clev)
    lon_up = jnp.asarray(lon_refine.T, BF16)
    lon_down = jnp.asarray(lon_refine, BF16)
    mix_up = jnp.asarray(np.concatenate([mix, mix], axis=1), BF16)
    mix_down = jnp.asarray(mix.T, BF16)
    pick = np.zeros((512, 512), np.float32)
    for r in range(4):
        for q in range(128):
            pick[4 * q + r, 128 * r + q] = 1.0
    pick = jnp.asarray(pick, BF16)
    order = np.eye(part * rows).reshape(part, rows, part, rows).transpose(1, 0, 2, 3)
    order = jnp.asarray(order.reshape(part * rows, part * rows), BF16)

    own = controls.reshape(members * clev, clon)
    low_high = [lax.ppermute(own, "lat", across), lax.ppermute(own, "lat", mates)]
    pert = perturbations.reshape(members, lev * band, lon)

    tail = jnp.concatenate([fine_frac, fine_source.astype(F32)])
    tail = jnp.pad(tail[None], ((0, 3), (0, fine_lon - 2 * rows)))
    spots = 8 * PASSES + 2 * HALO + 4
    coef, own_weight, buf_a, buf_b = pl.pallas_call(
        prepare_kernel,
        name="prepare",
        grid_spec=pltpu.PrefetchScalarGridSpec(
            num_scalar_prefetch=1,
            grid=(1,),
            in_specs=[
                pl.BlockSpec((part, rows, fine_lon), lambda i, p: (p[2], 0, 0)),
                pl.BlockSpec((rows, fine_lon), lambda i, p: (0, 0)),
                pl.BlockSpec((rows, fine_lon), lambda i, p: (0, 0)),
                pl.BlockSpec((4, fine_lon), lambda i, p: (0, 0)),
                pl.BlockSpec((512, 512), lambda i, p: (0, 0)),
                pl.BlockSpec((part * rows, part * rows), lambda i, p: (0, 0)),
            ],
            out_specs=[
                pl.BlockSpec((2 * rows, fine_lon), lambda i, p: (0, 0)),
                pl.BlockSpec((rows, part, fine_lon), lambda i, p: (0, 0, 0)),
                pl.BlockSpec((spots, fine_lon), lambda i, p: (0, 0)),
                pl.BlockSpec((spots, fine_lon), lambda i, p: (0, 0)),
            ],
        ),
        out_shape=[
            jax.ShapeDtypeStruct((2 * rows, fine_lon), F32),
            jax.ShapeDtypeStruct((rows, part, fine_lon), F32),
            jax.ShapeDtypeStruct((spots, fine_lon), F32),
            jax.ShapeDtypeStruct((spots, fine_lon), F32),
        ],
        compiler_params=pltpu.CompilerParams(vmem_limit_bytes=48 * 2**20),
    )(place, precision_weight, north_coef, east_coef, tail, pick, order)
    far_b = lax.ppermute(buf_b, "lat", across)
    far_a = lax.ppermute(buf_a, "lat", mates)

    local_sum = call(
        raise_kernel, "raise", (ranks, part * band, lon),
        [(3 * members * clev, clon), (lev * band, lon)],
        [place], [own, low_high[1], low_high[0], pert, lon_up, mix_up],
    )
    parts = lax.all_to_all(local_sum, "mem", 0, 0, tiled=True)
    mine = call(total_kernel, "total", (band * part, lon), [(band * part * lon // 128, 128)], [], [parts])
    mate = lax.ppermute(mine, "lat", mates)
    pair = jnp.concatenate([mine, mate], axis=0)
    up_pair = lax.ppermute(pair, "lat", up_two)
    down_pair = lax.ppermute(pair, "lat", down_two)

    n = rows + 2 * HALO
    north, east, west, weight = call(
        assemble_kernel, "assemble",
        [(n, 8, fine_lon), (n, 8, fine_lon), (n, 8, lon), (rows + 2 * PASSES, 8, fine_lon)],
        [], [place], [coef, own_weight, far_a, far_b],
    )
    at = 8 * PASSES + 2 * HALO
    extra_a = far_a[at : at + 1, : 2 * rows]
    extra_b = far_b[at : at + 1, : 2 * rows]
    piece = (band * part, lon)
    keep, send_a, send_b = call(
        fine_kernel, "fine", [piece, piece, piece],
        [(5 * band, 8, lon), (n, 8, fine_lon), (3 * band, 8, lon)],
        [place, fine_source, fine_frac, extra_a, extra_b],
        [mine, mate, up_pair, down_pair, north, east, west, weight],
    )
    got_b = lax.ppermute(send_b, "lat", across)
    got_a = lax.ppermute(send_a, "lat", mates)
    copies = call(
        copies_kernel, "copies", (ranks, band * part, lon),
        [(band * part * lon // 128, 128)], [], [keep, got_a, got_b]
    )
    adjoint = lax.all_to_all(copies, "mem", 0, 0, tiled=True)
    flat = (members * clev, clon)
    result, send_a, send_b = call(
        lower_kernel, "lower", [flat, flat, flat], [(3 * members * clev, lon)],
        [place], [pert, adjoint, mix_down, lon_down],
    )
    got_b = lax.ppermute(send_b, "lat", across)
    got_a = lax.ppermute(send_a, "lat", mates)
    return controls + (result + got_a + got_b).reshape(controls.shape)


def solution(mesh):
    in_specs = (
        P("mem", None, "lat", None),
        P("mem", None, "lat", None),
        P(None, "lat", None),
        P("lat", None),
        P("lat", None),
        P("lat"),
        P("lat"),
    )
    out_specs = P("mem", None, "lat", None)
    return jax.shard_map(body, mesh=mesh, in_specs=in_specs, out_specs=out_specs, check_vma=False)
```

```python
import jax
import jax.numpy as jnp
import numpy as np
from jax import lax
from jax.experimental import pallas as pl
from jax.experimental.pallas import tpu as pltpu
from jax.sharding import PartitionSpec as P

PASSES = 5
REACH = 4
HALO = 2 * PASSES
VMEM_LIMIT = 24 * 2**20
F32 = jnp.float32
BF16 = jnp.bfloat16

PHASES = np.array(
    [[0.375, 0.625, 0.0], [0.125, 0.875, 0.0], [0.0, 0.875, 0.125], [0.0, 0.625, 0.375]]
)


def refine_matrix(count, periodic):
    matrix = np.zeros((4 * count, count), np.float32)
    for q in range(count):
        for r in range(4):
            for step in range(3):
                source = q + step - 1
                source = source % count if periodic else min(max(source, 0), count - 1)
                matrix[4 * q + r, source] += PHASES[r, step]
    return matrix


def split2(x):
    hi = x.astype(BF16)
    lo = (x - hi.astype(F32)).astype(BF16)
    return hi, lo


def dot(a, b):
    return jnp.dot(a, b, preferred_element_type=F32)


def prepare_kernel(
    place, weight, north, east, extra, select, order, coef, own_weight, buf_a, buf_b, level_weight, sem
):
    odd = place[0] % 2
    levels, rows, lon = level_weight.shape
    fetch = pltpu.make_async_copy(weight.at[pl.ds(place[2] * levels, levels)], level_weight, sem)
    fetch.start()
    stacked = jnp.concatenate([north[...], east[...]], axis=0)
    hi = stacked.astype(BF16)
    rest = stacked - hi.astype(F32)
    mid = rest.astype(BF16)
    low = (rest - mid.astype(F32)).astype(BF16)
    fetch.wait()
    values = dot(order[...], level_weight[...].reshape(levels * rows, lon)).astype(BF16)
    everything = jnp.concatenate([values, hi, mid, low], axis=0)
    many = levels * rows
    quarter = lon // 4
    for c in range(lon // 512):
        moved = dot(everything[:, 512 * c : 512 * c + 512], select[...])
        wpart = moved[:many]
        cpart = moved[many : many + 2 * rows] + moved[many + 2 * rows : many + 4 * rows]
        cpart = cpart + moved[many + 4 * rows :]
        for r in range(4):
            to = slice(quarter * r + 128 * c, quarter * r + 128 * c + 128)
            frm = slice(128 * r, 128 * r + 128)
            coef[:, to] = cpart[:, frm]
            own_weight[:, :, to] = wpart[:, frm].reshape(rows, levels, 128)

    def fill(buf, upper):
        first = rows - PASSES if upper else 0
        for k in range(PASSES):
            buf[8 * k : 8 * k + 8, :] = own_weight[first + k]
        first = rows - HALO if upper else 0
        base = 8 * PASSES
        buf[base : base + HALO, :] = coef[first : first + HALO, :]
        buf[base + HALO : base + 2 * HALO, :] = coef[rows + first : rows + first + HALO, :]
        buf[base + 2 * HALO :, :] = extra[...]

    @pl.when(odd == 0)
    def _():
        fill(buf_a, True)
        fill(buf_b, False)

    @pl.when(odd == 1)
    def _():
        fill(buf_a, False)
        fill(buf_b, True)


def assemble_kernel(place, coef, own_weight, got_a, got_b, north, east, west, weight):
    lat = place[0]
    odd = lat % 2
    rows = own_weight.shape[0]
    quarter = coef.shape[1] // 4

    def put(i, nrow, erow):
        shape = (8, coef.shape[1])
        north[i] = jnp.broadcast_to(nrow, shape)
        spread = jnp.broadcast_to(erow, shape)
        east[i] = spread
        west[i] = pltpu.roll(spread[:, 3 * quarter :], 1, axis=1)

    for k in range(rows):
        put(HALO + k, coef[k : k + 1, :], coef[rows + k : rows + k + 1, :])
        weight[PASSES + k] = own_weight[k]

    def side(buf, start, wstart):
        base = 8 * PASSES
        for k in range(HALO):
            put(start + k, buf[base + k : base + k + 1, :], buf[base + HALO + k : base + HALO + k + 1, :])
        for k in range(PASSES):
            weight[wstart + k] = buf[8 * k : 8 * k + 8, :]

    @pl.when(odd == 0)
    def _():
        side(got_b, 0, 0)
        side(got_a, HALO + rows, PASSES + rows)

    @pl.when(odd == 1)
    def _():
        side(got_a, 0, 0)
        side(got_b, HALO + rows, PASSES + rows)

    @pl.when(lat == 0)
    def _():
        north[HALO - 1] = jnp.zeros(north.shape[1:], F32)


def arrange_kernel(pert, out):
    members, lev, band, _ = pert.shape
    for m in range(members):
        values = pert[m].astype(F32)
        for k in range(lev):
            out[m, band * k : band * k + band, :] = values[k]


def raise_kernel(place, own, got_a, got_b, pert, lon_up, mix, out, x, acc):
    lat, last = place[0], place[1] - 1
    odd = lat % 2
    members = pert.shape[0]
    lev = own.shape[0] // members

    def put(step, ref):
        for m in range(members):
            at = (3 * m + step) * lev
            x[at : at + lev, :] = ref[m * lev : m * lev + lev, :]

    put(1, own)

    @pl.when(lat == 0)
    def _():
        put(0, own)

    @pl.when((lat > 0) & (odd == 0))
    def _():
        put(0, got_b)

    @pl.when(odd == 1)
    def _():
        put(0, got_a)

    @pl.when(lat == last)
    def _():
        put(2, own)

    @pl.when((lat < last) & (odd == 1))
    def _():
        put(2, got_b)

    @pl.when(odd == 0)
    def _():
        put(2, got_a)

    hi, lo = split2(x[...])
    wide = dot(hi, lon_up[...]) + dot(lo, lon_up[...])
    for m in range(members):
        hi, lo = split2(wide[3 * lev * m : 3 * lev * (m + 1), :])
        field = dot(mix[...], jnp.concatenate([hi, lo], axis=0))
        term = field * pert[m]
        if m == 0:
            acc[...] = term
        elif m < members - 1:
            acc[...] += term
        else:
            out[...] = (acc[...] + term).reshape(out.shape)


def total_kernel(parts, out, sums):
    count, n, lon = parts.shape
    total = parts[0]
    for k in range(1, count):
        total = total + parts[k]
    rows = n // 8
    for c in range(lon // 128):
        lanes = slice(128 * c, 128 * c + 128)
        sums[n * c : n * c + n, :] = total[:, lanes]
        for row in range(rows):
            out[8 * row : 8 * row + 8, lanes] = sums[pl.ds(n * c + row, 8, stride=rows), :]


def fine_kernel(
    place, source, frac, extra_a, extra_b, own, mate, near_pair, far_pair,
    north, east, west, weight, keep, send_a, send_b, mid, v, acc,
):
    lat, last = place[0], place[1] - 1
    odd = lat % 2
    lon = own.shape[1]
    rows = source.shape[0]
    n = rows + 2 * HALO
    band = own.shape[0] // 8

    def bring(slot, ref, start):
        for k in range(band):
            mid[slot * band + k] = ref[start + 8 * k : start + 8 * k + 8, :]

    half = own.shape[0]
    bring(2, own, 0)

    def gather(even, up_pair, down_pair):
        bring(0, up_pair, 0)
        bring(4, down_pair, 0)
        if even:
            bring(1, up_pair, half)
            bring(3, mate, 0)
        else:
            bring(1, mate, 0)
            bring(3, down_pair, half)

    turn = lat % 4
    for case in range(4):

        @pl.when(turn == case)
        def _(case=case):
            if case < 2:
                gather(case % 2 == 0, far_pair, near_pair)
            else:
                gather(case % 2 == 0, near_pair, far_pair)

    origin = (lat - 2) * band
    for i in range(n):
        k = i - HALO
        if k < 0:
            k += rows
            f = jnp.where(odd == 1, extra_a[0, k], extra_b[0, k])
            s = jnp.where(odd == 1, extra_a[0, rows + k], extra_b[0, rows + k]).astype(jnp.int32)
            valid = jnp.where(lat > 0, 1.0, 0.0)
        elif k >= rows:
            k -= rows
            f = jnp.where(odd == 0, extra_a[0, k], extra_b[0, k])
            s = jnp.where(odd == 0, extra_a[0, rows + k], extra_b[0, rows + k]).astype(jnp.int32)
            valid = jnp.where(lat < last, 1.0, 0.0)
        else:
            f, s, valid = frac[k], source[k], None
        s = jnp.clip(s - origin, 0, 5 * band - 2)
        below, above = 1.0 - f, f
        if valid is not None:
            below, above = below * valid, above * valid
        cur = below * mid[s] + above * mid[s + 1]
        prev = pltpu.roll(cur, 1, axis=1)
        nxt = pltpu.roll(cur, lon - 1, axis=1)
        v[i, :, 0:lon] = 0.375 * prev + 0.625 * cur
        v[i, :, lon : 2 * lon] = 0.125 * prev + 0.875 * cur
        v[i, :, 2 * lon : 3 * lon] = 0.875 * cur + 0.125 * nxt
        v[i, :, 3 * lon : 4 * lon] = 0.625 * cur + 0.375 * nxt

    inside_top = jnp.where(lat < last, 1.0, 0.0)

    def cut(r):
        return slice(r * lon, r * lon + lon)

    def sweep(first, stop):
        def flux(i, here, there):
            return [north[i, :, cut(r)] * (there[r] - here[r]) for r in range(4)]

        before = [v[first - 1, :, cut(r)] for r in range(4)]
        here = [v[first, :, cut(r)] for r in range(4)]
        low = flux(first - 1, before, here)
        for i in range(first, stop):
            there = [v[i + 1, :, cut(r)] for r in range(4)]
            high = flux(i, here, there)
            if i == HALO + rows:
                low = [inside_top * x for x in low]
            right = pltpu.roll(here[0], lon - 1, axis=1)
            left = pltpu.roll(here[3], 1, axis=1)
            side = [
                east[i, :, cut(r)] * ((here[r + 1] if r < 3 else right) - here[r]) for r in range(4)
            ]
            back = [west[i] * (here[0] - left)] + side[:3]
            for r in range(4):
                v[i, :, cut(r)] = here[r] + ((high[r] - low[r]) + (side[r] - back[r]))
            low, here = high, there

    def first_pass(_, carry):
        sweep(1, n - 1)
        return carry

    lax.fori_loop(0, PASSES, first_pass, 0)

    def scale(k, carry):
        v[PASSES + k] = weight[k] * v[PASSES + k]
        return carry

    lax.fori_loop(0, rows + 2 * PASSES, scale, 0)

    def second_pass(_, carry):
        sweep(PASSES + 1, n - PASSES - 1)
        return carry

    lax.fori_loop(0, PASSES, second_pass, 0)

    acc[...] = jnp.zeros(acc.shape, F32)
    base = (lat - 1) * band
    for k in range(rows):
        o = [v[HALO + k, :, cut(r)] for r in range(4)]
        ahead = pltpu.roll(0.375 * o[0] + 0.125 * o[1], lon - 1, axis=1)
        behind = pltpu.roll(0.125 * o[2] + 0.375 * o[3], 1, axis=1)
        g = 0.625 * (o[0] + o[3]) + 0.875 * (o[1] + o[2]) + (ahead + behind)
        s = jnp.clip(source[k] - base, 0, 3 * band - 2)
        f = frac[k]
        acc[s] += (1.0 - f) * g
        acc[s + 1] += f * g
    for k in range(band):
        keep[8 * k : 8 * k + 8, :] = acc[band + k]

    def give(ref, slot):
        for k in range(band):
            ref[8 * k : 8 * k + 8, :] = acc[slot * band + k]

    @pl.when(odd == 0)
    def _():
        give(send_a, 2)
        give(send_b, 0)

    @pl.when(odd == 1)
    def _():
        give(send_a, 0)
        give(send_b, 2)


def copies_kernel(keep, got_a, got_b, out, sums):
    count, n, lon = out.shape
    rows = n // 8
    total = keep[...] + got_a[...] + got_b[...]
    for c in range(lon // 128):
        lanes = slice(128 * c, 128 * c + 128)
        for row in range(rows):
            sums[pl.ds(n * c + row, 8, stride=rows), :] = total[8 * row : 8 * row + 8, lanes]
        value = sums[n * c : n * c + n, :]
        for k in range(count):
            out[k, :, lanes] = value


def lower_kernel(place, controls, pert, adjoint, mix_t, lon_down, own, send_a, send_b, wide):
    lat, last = place[0], place[1] - 1
    odd = lat % 2
    members = pert.shape[0]
    lev = own.shape[0] // members
    field = adjoint[...].reshape(pert.shape[1], pert.shape[2])
    for m in range(members):
        hi, lo = split2(field * pert[m])
        wide[3 * lev * m : 3 * lev * (m + 1), :] = dot(mix_t[...], hi) + dot(mix_t[...], lo)
    hi, lo = split2(wide[...])
    narrow = dot(hi, lon_down[...]) + dot(lo, lon_down[...])
    at_first = jnp.where(lat == 0, 1.0, 0.0)
    at_last = jnp.where(lat == last, 1.0, 0.0)
    is_odd = jnp.where(odd == 1, 1.0, 0.0)
    for m in range(members):
        at = 3 * lev * m
        low = narrow[at : at + lev]
        mine = narrow[at + lev : at + 2 * lev]
        high = narrow[at + 2 * lev : at + 3 * lev]
        to = slice(m * lev, m * lev + lev)
        own[to, :] = controls[to, :] + mine + at_first * low + at_last * high
        low = (1.0 - at_first) * low
        high = (1.0 - at_last) * high
        send_a[to, :] = is_odd * low + (1.0 - is_odd) * high
        send_b[to, :] = is_odd * high + (1.0 - is_odd) * low


def vmem():
    return pl.BlockSpec(memory_space=pltpu.VMEM)


def smem():
    return pl.BlockSpec(memory_space=pltpu.SMEM)


def call(kernel, name, outs, scratch, scalars, vectors):
    many = isinstance(outs, list)
    shapes = [jax.ShapeDtypeStruct(s, F32) for s in (outs if many else [outs])]
    return pl.pallas_call(
        kernel,
        name=name,
        out_shape=shapes if many else shapes[0],
        in_specs=[smem()] * len(scalars) + [vmem()] * len(vectors),
        out_specs=[vmem()] * len(shapes) if many else vmem(),
        scratch_shapes=[pltpu.VMEM(s, F32) for s in scratch],
        compiler_params=pltpu.CompilerParams(vmem_limit_bytes=VMEM_LIMIT),
    )(*scalars, *vectors)


def body(controls, perturbations, precision_weight, north_coef, east_coef, fine_source, fine_frac):
    lat = lax.axis_index("lat")
    count = lax.axis_size("lat")
    mem = lax.axis_index("mem")
    ranks = lax.axis_size("mem")
    members, clev, _, clon = controls.shape
    lev, band, lon = perturbations.shape[1:]
    rows, fine_lon = north_coef.shape
    part = lev // ranks

    mates = [(i, i ^ 1) for i in range(count)]
    across = [(i, (i + 1) % count if i % 2 else (i - 1) % count) for i in range(count)]
    near_chips = [(i, i ^ 2) for i in range(count)]
    far_chips = [(i, (i + 2) % count if i & 2 else (i - 2) % count) for i in range(count)]

    place = jnp.stack([lat, jnp.int32(count), mem]).astype(jnp.int32)
    lon_refine = refine_matrix(clon, True)
    lev_refine = refine_matrix(clev, False)
    mix = np.einsum("vl,rt->vrtl", lev_refine, PHASES).reshape(lev * band, 3 * clev)
    lon_up = jnp.asarray(lon_refine.T, BF16)
    lon_down = jnp.asarray(lon_refine, BF16)
    mix_up = jnp.asarray(np.concatenate([mix, mix], axis=1), BF16)
    mix_down = jnp.asarray(mix.T, BF16)
    pick = np.zeros((512, 512), np.float32)
    for r in range(4):
        for q in range(128):
            pick[4 * q + r, 128 * r + q] = 1.0
    pick = jnp.asarray(pick, BF16)
    order = np.eye(part * rows).reshape(part, rows, part, rows).transpose(1, 0, 2, 3)
    order = jnp.asarray(order.reshape(part * rows, part * rows), BF16)

    own = controls.reshape(members * clev, clon)
    low_high = [lax.ppermute(own, "lat", across), lax.ppermute(own, "lat", mates)]
    pert = call(arrange_kernel, "arrange", (members, lev * band, lon), [], [], [perturbations])

    tail = jnp.concatenate([fine_frac, fine_source.astype(F32)])
    tail = jnp.pad(tail[None], ((0, 3), (0, fine_lon - 2 * rows)))
    spots = 8 * PASSES + 2 * HALO + 4
    coef, own_weight, buf_a, buf_b = pl.pallas_call(
        prepare_kernel,
        name="prepare",
        out_shape=[
            jax.ShapeDtypeStruct((2 * rows, fine_lon), F32),
            jax.ShapeDtypeStruct((rows, part, fine_lon), F32),
            jax.ShapeDtypeStruct((spots, fine_lon), F32),
            jax.ShapeDtypeStruct((spots, fine_lon), F32),
        ],
        in_specs=[smem(), pl.BlockSpec(memory_space=pltpu.HBM)] + [vmem()] * 5,
        out_specs=[vmem()] * 4,
        scratch_shapes=[pltpu.VMEM((part, rows, fine_lon), BF16), pltpu.SemaphoreType.DMA(())],
        compiler_params=pltpu.CompilerParams(vmem_limit_bytes=VMEM_LIMIT),
    )(place, precision_weight, north_coef, east_coef, tail, pick, order)
    far_b = lax.ppermute(buf_b, "lat", across)
    far_a = lax.ppermute(buf_a, "lat", mates)

    local_sum = call(
        raise_kernel, "raise", (ranks, part * band, lon),
        [(3 * members * clev, clon), (lev * band, lon)],
        [place], [own, low_high[1], low_high[0], pert, lon_up, mix_up],
    )
    parts = lax.all_to_all(local_sum, "mem", 0, 0, tiled=True)
    mine = call(total_kernel, "total", (band * part, lon), [(band * part * lon // 128, 128)], [], [parts])
    mate = lax.ppermute(mine, "lat", mates)
    pair = jnp.concatenate([mine, mate], axis=0)
    far_pair = lax.ppermute(pair, "lat", far_chips)
    near_pair = lax.ppermute(pair, "lat", near_chips)

    n = rows + 2 * HALO
    north, east, west, weight = call(
        assemble_kernel, "assemble",
        [(n, 8, fine_lon), (n, 8, fine_lon), (n, 8, lon), (rows + 2 * PASSES, 8, fine_lon)],
        [], [place], [coef, own_weight, far_a, far_b],
    )
    at = 8 * PASSES + 2 * HALO
    extra_a = far_a[at : at + 1, : 2 * rows]
    extra_b = far_b[at : at + 1, : 2 * rows]
    piece = (band * part, lon)
    keep, send_a, send_b = call(
        fine_kernel, "fine", [piece, piece, piece],
        [(5 * band, 8, lon), (n, 8, fine_lon), (3 * band, 8, lon)],
        [place, fine_source, fine_frac, extra_a, extra_b],
        [mine, mate, near_pair, far_pair, north, east, west, weight],
    )
    got_b = lax.ppermute(send_b, "lat", across)
    got_a = lax.ppermute(send_a, "lat", mates)
    copies = call(
        copies_kernel, "copies", (ranks, band * part, lon),
        [(band * part * lon // 128, 128)], [], [keep, got_a, got_b]
    )
    adjoint = lax.all_to_all(copies, "mem", 0, 0, tiled=True)
    flat = (members * clev, clon)
    result, send_a, send_b = call(
        lower_kernel, "lower", [flat, flat, flat], [(3 * members * clev, lon)],
        [place], [own, pert, adjoint, mix_down, lon_down],
    )
    got_b = lax.ppermute(send_b, "lat", across)
    got_a = lax.ppermute(send_a, "lat", mates)
    return (result + got_a + got_b).reshape(controls.shape)


def solution(mesh):
    in_specs = (
        P("mem", None, "lat", None),
        P("mem", None, "lat", None),
        P(None, "lat", None),
        P("lat", None),
        P("lat", None),
        P("lat"),
        P("lat"),
    )
    out_specs = P("mem", None, "lat", None)
    return jax.shard_map(body, mesh=mesh, in_specs=in_specs, out_specs=out_specs, check_vma=False)
```

```python
import jax
import jax.numpy as jnp
import numpy as np
from jax import lax
from jax.experimental import pallas as pl
from jax.experimental.pallas import tpu as pltpu
from jax.sharding import PartitionSpec as P

PASSES = 5
REACH = 4
HALO = 2 * PASSES
VMEM_LIMIT = 24 * 2**20
F32 = jnp.float32
BF16 = jnp.bfloat16

PHASES = np.array(
    [[0.375, 0.625, 0.0], [0.125, 0.875, 0.0], [0.0, 0.875, 0.125], [0.0, 0.625, 0.375]]
)


def refine_matrix(count, periodic):
    matrix = np.zeros((4 * count, count), np.float32)
    for q in range(count):
        for r in range(4):
            for step in range(3):
                source = q + step - 1
                source = source % count if periodic else min(max(source, 0), count - 1)
                matrix[4 * q + r, source] += PHASES[r, step]
    return matrix


def split2(x):
    hi = x.astype(BF16)
    lo = (x - hi.astype(F32)).astype(BF16)
    return hi, lo


def dot(a, b):
    return jnp.dot(a, b, preferred_element_type=F32)


def prepare_kernel(
    place, source, frac, weight, north_all, east_all, select_all, order_all,
    coef, own_weight, buf_a, buf_b, level_weight, north, east, select, order, extra, sems,
):
    odd = place[0] % 2
    levels, rows, lon = level_weight.shape
    copies = [
        pltpu.make_async_copy(north_all, north, sems.at[0]),
        pltpu.make_async_copy(east_all, east, sems.at[1]),
        pltpu.make_async_copy(
            weight.at[pl.ds(place[2] * levels, levels)], level_weight, sems.at[2]
        ),
        pltpu.make_async_copy(order_all, order, sems.at[3]),
        pltpu.make_async_copy(select_all, select, sems.at[4]),
    ]
    for copy in copies:
        copy.start()
    lane = lax.broadcasted_iota(jnp.int32, (4, 128), 1)
    tail = jnp.zeros((4, 128), F32)
    for k in range(rows):
        tail = jnp.where(lane == k, frac[k], tail)
        tail = jnp.where(lane == rows + k, source[k].astype(F32), tail)
    extra[...] = jnp.zeros(extra.shape, F32)
    extra[:, 0:128] = tail
    copies[0].wait()
    copies[1].wait()
    stacked = jnp.concatenate([north[...], east[...]], axis=0)
    hi = stacked.astype(BF16)
    rest = stacked - hi.astype(F32)
    mid = rest.astype(BF16)
    low = (rest - mid.astype(F32)).astype(BF16)
    copies[2].wait()
    copies[3].wait()
    values = dot(order[...], level_weight[...].reshape(levels * rows, lon)).astype(BF16)
    everything = jnp.concatenate([values, hi, mid, low], axis=0)
    copies[4].wait()
    many = levels * rows
    quarter = lon // 4
    for c in range(lon // 512):
        moved = dot(everything[:, 512 * c : 512 * c + 512], select[...])
        wpart = moved[:many]
        cpart = moved[many : many + 2 * rows] + moved[many + 2 * rows : many + 4 * rows]
        cpart = cpart + moved[many + 4 * rows :]
        for r in range(4):
            to = slice(quarter * r + 128 * c, quarter * r + 128 * c + 128)
            frm = slice(128 * r, 128 * r + 128)
            coef[:, to] = cpart[:, frm]
            own_weight[:, :, to] = wpart[:, frm].reshape(rows, levels, 128).astype(BF16)

    def fill(buf, upper):
        first = rows - PASSES if upper else 0
        for k in range(PASSES):
            buf[8 * k : 8 * k + 8, :] = own_weight[first + k].astype(F32)
        first = rows - HALO if upper else 0
        base = 8 * PASSES
        buf[base : base + HALO, :] = coef[first : first + HALO, :]
        buf[base + HALO : base + 2 * HALO, :] = coef[rows + first : rows + first + HALO, :]
        buf[base + 2 * HALO :, :] = extra[...]

    @pl.when(odd == 0)
    def _():
        fill(buf_a, True)
        fill(buf_b, False)

    @pl.when(odd == 1)
    def _():
        fill(buf_a, False)
        fill(buf_b, True)


def assemble_kernel(place, coef, own_weight, got_a, got_b, north, east, west, weight):
    lat = place[0]
    odd = lat % 2
    rows = own_weight.shape[0]
    quarter = coef.shape[1] // 4

    def put(i, nrow, erow):
        shape = (8, coef.shape[1])
        north[i] = jnp.broadcast_to(nrow, shape)
        spread = jnp.broadcast_to(erow, shape)
        east[i] = spread
        west[i] = pltpu.roll(spread[:, 3 * quarter :], 1, axis=1)

    for k in range(rows):
        put(HALO + k, coef[k : k + 1, :], coef[rows + k : rows + k + 1, :])
        weight[PASSES + k] = own_weight[k].astype(F32)

    def side(buf, start, wstart):
        base = 8 * PASSES
        for k in range(HALO):
            put(start + k, buf[base + k : base + k + 1, :], buf[base + HALO + k : base + HALO + k + 1, :])
        for k in range(PASSES):
            weight[wstart + k] = buf[8 * k : 8 * k + 8, :]

    @pl.when(odd == 0)
    def _():
        side(got_b, 0, 0)
        side(got_a, HALO + rows, PASSES + rows)

    @pl.when(odd == 1)
    def _():
        side(got_a, 0, 0)
        side(got_b, HALO + rows, PASSES + rows)

    @pl.when(lat == 0)
    def _():
        north[HALO - 1] = jnp.zeros(north.shape[1:], F32)


def raise_kernel(
    place, got_a, got_b, own_all, lon_all, mix_all, stored, out, pert, x, acc, raw, flat, own, lon_up,
    mix, sems,
):
    lat, last = place[0], place[1] - 1
    odd = lat % 2
    members, levels, band, _ = raw.shape
    lev = own.shape[0] // members
    small = [
        pltpu.make_async_copy(own_all, own, sems.at[members]),
        pltpu.make_async_copy(lon_all, lon_up, sems.at[members + 1]),
        pltpu.make_async_copy(mix_all, mix, sems.at[members + 2]),
    ]
    copies = [pltpu.make_async_copy(stored.at[m], raw.at[m], sems.at[m]) for m in range(members)]
    for copy in small + copies:
        copy.start()
    for copy in small:
        copy.wait()

    def put(step, ref):
        for m in range(members):
            at = (3 * m + step) * lev
            x[at : at + lev, :] = ref[m * lev : m * lev + lev, :]

    put(1, own)

    @pl.when(lat == 0)
    def _():
        put(0, own)

    @pl.when((lat > 0) & (odd == 0))
    def _():
        put(0, got_b)

    @pl.when(odd == 1)
    def _():
        put(0, got_a)

    @pl.when(lat == last)
    def _():
        put(2, own)

    @pl.when((lat < last) & (odd == 1))
    def _():
        put(2, got_b)

    @pl.when(odd == 0)
    def _():
        put(2, got_a)

    hi, lo = split2(x[...])
    wide = dot(hi, lon_up[...]) + dot(lo, lon_up[...])
    for m in range(members):
        copies[m].wait()
        values = raw[m].astype(F32)
        for k in range(levels):
            flat[band * k : band * k + band, :] = values[k]
        spread = flat[...]
        pert[m] = spread.astype(BF16)
        hi, lo = split2(wide[3 * lev * m : 3 * lev * (m + 1), :])
        field = dot(mix[...], jnp.concatenate([hi, lo], axis=0))
        term = field * spread
        if m == 0:
            acc[...] = term
        elif m < members - 1:
            acc[...] += term
        else:
            out[...] = (acc[...] + term).reshape(out.shape)


def total_kernel(parts, out, sums):
    count, n, lon = parts.shape
    total = parts[0]
    for k in range(1, count):
        total = total + parts[k]
    rows = n // 8
    for c in range(lon // 128):
        lanes = slice(128 * c, 128 * c + 128)
        sums[n * c : n * c + n, :] = total[:, lanes]
        for row in range(rows):
            out[8 * row : 8 * row + 8, lanes] = sums[pl.ds(n * c + row, 8, stride=rows), :]


def join_kernel(mine, mate, out):
    half = mine.shape[0]
    out[:half] = mine[...]
    out[half:] = mate[...]


def fine_kernel(
    place, source, frac, far_a, far_b, own, mate, near_pair, far_pair,
    north, east, west, weight, keep, send_a, send_b, mid, v, acc, extra_a, extra_b, sems,
):
    at = 8 * PASSES + 2 * HALO
    copies = [
        pltpu.make_async_copy(far_a.at[at : at + 1, 0:128], extra_a, sems.at[0]),
        pltpu.make_async_copy(far_b.at[at : at + 1, 0:128], extra_b, sems.at[1]),
    ]
    for copy in copies:
        copy.start()
    lat, last = place[0], place[1] - 1
    odd = lat % 2
    lon = own.shape[1]
    rows = source.shape[0]
    n = rows + 2 * HALO
    band = own.shape[0] // 8

    def bring(slot, ref, start):
        for k in range(band):
            mid[slot * band + k] = ref[start + 8 * k : start + 8 * k + 8, :]

    half = own.shape[0]
    bring(2, own, 0)

    def gather(even, up_pair, down_pair):
        bring(0, up_pair, 0)
        bring(4, down_pair, 0)
        if even:
            bring(1, up_pair, half)
            bring(3, mate, 0)
        else:
            bring(1, mate, 0)
            bring(3, down_pair, half)

    turn = lat % 4
    for case in range(4):

        @pl.when(turn == case)
        def _(case=case):
            if case < 2:
                gather(case % 2 == 0, far_pair, near_pair)
            else:
                gather(case % 2 == 0, near_pair, far_pair)

    for copy in copies:
        copy.wait()
    origin = (lat - 2) * band
    for i in range(n):
        k = i - HALO
        if k < 0:
            k += rows
            f = jnp.where(odd == 1, extra_a[0, k], extra_b[0, k])
            s = jnp.where(odd == 1, extra_a[0, rows + k], extra_b[0, rows + k]).astype(jnp.int32)
            valid = jnp.where(lat > 0, 1.0, 0.0)
        elif k >= rows:
            k -= rows
            f = jnp.where(odd == 0, extra_a[0, k], extra_b[0, k])
            s = jnp.where(odd == 0, extra_a[0, rows + k], extra_b[0, rows + k]).astype(jnp.int32)
            valid = jnp.where(lat < last, 1.0, 0.0)
        else:
            f, s, valid = frac[k], source[k], None
        s = jnp.clip(s - origin, 0, 5 * band - 2)
        below, above = 1.0 - f, f
        if valid is not None:
            below, above = below * valid, above * valid
        cur = below * mid[s] + above * mid[s + 1]
        prev = pltpu.roll(cur, 1, axis=1)
        nxt = pltpu.roll(cur, lon - 1, axis=1)
        v[i, :, 0:lon] = 0.375 * prev + 0.625 * cur
        v[i, :, lon : 2 * lon] = 0.125 * prev + 0.875 * cur
        v[i, :, 2 * lon : 3 * lon] = 0.875 * cur + 0.125 * nxt
        v[i, :, 3 * lon : 4 * lon] = 0.625 * cur + 0.375 * nxt

    inside_top = jnp.where(lat < last, 1.0, 0.0)

    def cut(r):
        return slice(r * lon, r * lon + lon)

    def sweep(first, stop):
        def flux(i, here, there):
            return [north[i, :, cut(r)] * (there[r] - here[r]) for r in range(4)]

        before = [v[first - 1, :, cut(r)] for r in range(4)]
        here = [v[first, :, cut(r)] for r in range(4)]
        low = flux(first - 1, before, here)
        for i in range(first, stop):
            there = [v[i + 1, :, cut(r)] for r in range(4)]
            high = flux(i, here, there)
            if i == HALO + rows:
                low = [inside_top * x for x in low]
            right = pltpu.roll(here[0], lon - 1, axis=1)
            left = pltpu.roll(here[3], 1, axis=1)
            side = [
                east[i, :, cut(r)] * ((here[r + 1] if r < 3 else right) - here[r]) for r in range(4)
            ]
            back = [west[i] * (here[0] - left)] + side[:3]
            for r in range(4):
                v[i, :, cut(r)] = here[r] + ((high[r] - low[r]) + (side[r] - back[r]))
            low, here = high, there

    def first_pass(_, carry):
        sweep(1, n - 1)
        return carry

    lax.fori_loop(0, PASSES, first_pass, 0)

    def scale(k, carry):
        v[PASSES + k] = weight[k] * v[PASSES + k]
        return carry

    lax.fori_loop(0, rows + 2 * PASSES, scale, 0)

    def second_pass(_, carry):
        sweep(PASSES + 1, n - PASSES - 1)
        return carry

    lax.fori_loop(0, PASSES, second_pass, 0)

    acc[...] = jnp.zeros(acc.shape, F32)
    base = (lat - 1) * band
    for k in range(rows):
        o = [v[HALO + k, :, cut(r)] for r in range(4)]
        ahead = pltpu.roll(0.375 * o[0] + 0.125 * o[1], lon - 1, axis=1)
        behind = pltpu.roll(0.125 * o[2] + 0.375 * o[3], 1, axis=1)
        g = 0.625 * (o[0] + o[3]) + 0.875 * (o[1] + o[2]) + (ahead + behind)
        s = jnp.clip(source[k] - base, 0, 3 * band - 2)
        f = frac[k]
        acc[s] += (1.0 - f) * g
        acc[s + 1] += f * g
    for k in range(band):
        keep[8 * k : 8 * k + 8, :] = acc[band + k]

    def give(ref, slot):
        for k in range(band):
            ref[8 * k : 8 * k + 8, :] = acc[slot * band + k]

    @pl.when(odd == 0)
    def _():
        give(send_a, 2)
        give(send_b, 0)

    @pl.when(odd == 1)
    def _():
        give(send_a, 0)
        give(send_b, 2)


def copies_kernel(keep, got_a, got_b, out, sums):
    count, n, lon = out.shape
    rows = n // 8
    total = keep[...] + got_a[...] + got_b[...]
    for c in range(lon // 128):
        lanes = slice(128 * c, 128 * c + 128)
        for row in range(rows):
            sums[pl.ds(n * c + row, 8, stride=rows), :] = total[8 * row : 8 * row + 8, lanes]
        value = sums[n * c : n * c + n, :]
        for k in range(count):
            out[k, :, lanes] = value


def lower_kernel(place, controls, pert, adjoint, mix_t, lon_down, own, send_a, send_b, wide):
    lat, last = place[0], place[1] - 1
    odd = lat % 2
    members = pert.shape[0]
    lev = own.shape[0] // members
    field = adjoint[...].reshape(pert.shape[1], pert.shape[2])
    for m in range(members):
        hi, lo = split2(field * pert[m].astype(F32))
        wide[3 * lev * m : 3 * lev * (m + 1), :] = dot(mix_t[...], hi) + dot(mix_t[...], lo)
    hi, lo = split2(wide[...])
    narrow = dot(hi, lon_down[...]) + dot(lo, lon_down[...])
    at_first = jnp.where(lat == 0, 1.0, 0.0)
    at_last = jnp.where(lat == last, 1.0, 0.0)
    is_odd = jnp.where(odd == 1, 1.0, 0.0)
    for m in range(members):
        at = 3 * lev * m
        low = narrow[at : at + lev]
        mine = narrow[at + lev : at + 2 * lev]
        high = narrow[at + 2 * lev : at + 3 * lev]
        to = slice(m * lev, m * lev + lev)
        own[to, :] = controls[to, :] + mine + at_first * low + at_last * high
        low = (1.0 - at_first) * low
        high = (1.0 - at_last) * high
        send_a[to, :] = is_odd * low + (1.0 - is_odd) * high
        send_b[to, :] = is_odd * high + (1.0 - is_odd) * low


def vmem():
    return pl.BlockSpec(memory_space=pltpu.VMEM)


def anywhere():
    return pl.BlockSpec(memory_space=pl.ANY)


def in_hbm(x):
    return pltpu.with_memory_space_constraint(x, pltpu.HBM)


def smem():
    return pl.BlockSpec(memory_space=pltpu.SMEM)


def call(kernel, name, outs, scratch, scalars, vectors):
    many = isinstance(outs, list)
    shapes = [jax.ShapeDtypeStruct(s, F32) for s in (outs if many else [outs])]
    return pl.pallas_call(
        kernel,
        name=name,
        out_shape=shapes if many else shapes[0],
        in_specs=[smem()] * len(scalars) + [vmem()] * len(vectors),
        out_specs=[vmem()] * len(shapes) if many else vmem(),
        scratch_shapes=[pltpu.VMEM(s, F32) for s in scratch],
        compiler_params=pltpu.CompilerParams(vmem_limit_bytes=VMEM_LIMIT),
    )(*scalars, *vectors)


def body(controls, perturbations, precision_weight, north_coef, east_coef, fine_source, fine_frac):
    lat = lax.axis_index("lat")
    count = lax.axis_size("lat")
    mem = lax.axis_index("mem")
    ranks = lax.axis_size("mem")
    members, clev, _, clon = controls.shape
    lev, band, lon = perturbations.shape[1:]
    rows, fine_lon = north_coef.shape
    part = lev // ranks

    mates = [(i, i ^ 1) for i in range(count)]
    across = [(i, (i + 1) % count if i % 2 else (i - 1) % count) for i in range(count)]
    near_chips = [(i, i ^ 2) for i in range(count)]
    far_chips = [(i, (i + 2) % count if i & 2 else (i - 2) % count) for i in range(count)]

    place = jnp.stack([lat, jnp.int32(count), mem]).astype(jnp.int32)
    lon_refine = refine_matrix(clon, True)
    lev_refine = refine_matrix(clev, False)
    mix = np.einsum("vl,rt->vrtl", lev_refine, PHASES).reshape(lev * band, 3 * clev)
    lon_up = jnp.asarray(lon_refine.T, BF16)
    lon_down = jnp.asarray(lon_refine, BF16)
    mix_up = jnp.asarray(np.concatenate([mix, mix], axis=1), BF16)
    mix_down = jnp.asarray(mix.T, BF16)
    pick = np.zeros((512, 512), np.float32)
    for r in range(4):
        for q in range(128):
            pick[4 * q + r, 128 * r + q] = 1.0
    pick = jnp.asarray(pick, BF16)
    order = np.eye(part * rows).reshape(part, rows, part, rows).transpose(1, 0, 2, 3)
    order = jnp.asarray(order.reshape(part * rows, part * rows), BF16)

    own = controls.reshape(members * clev, clon)
    low_high = [lax.ppermute(own, "lat", across), lax.ppermute(own, "lat", mates)]

    spots = 8 * PASSES + 2 * HALO + 4
    coef, own_weight, buf_a, buf_b = pl.pallas_call(
        prepare_kernel,
        name="prepare",
        out_shape=[
            jax.ShapeDtypeStruct((2 * rows, fine_lon), F32),
            jax.ShapeDtypeStruct((rows, part, fine_lon), BF16),
            jax.ShapeDtypeStruct((spots, fine_lon), F32),
            jax.ShapeDtypeStruct((spots, fine_lon), F32),
        ],
        in_specs=[smem()] * 3 + [anywhere()] * 5,
        out_specs=[vmem()] * 4,
        scratch_shapes=[
            pltpu.VMEM((part, rows, fine_lon), BF16),
            pltpu.VMEM((rows, fine_lon), F32),
            pltpu.VMEM((rows, fine_lon), F32),
            pltpu.VMEM((512, 512), BF16),
            pltpu.VMEM((part * rows, part * rows), BF16),
            pltpu.VMEM((4, fine_lon), F32),
            pltpu.SemaphoreType.DMA((5,)),
        ],
        compiler_params=pltpu.CompilerParams(vmem_limit_bytes=VMEM_LIMIT),
    )(
        place, fine_source, fine_frac,
        *[in_hbm(x) for x in (precision_weight, north_coef, east_coef, pick, order)],
    )
    far_b = lax.ppermute(buf_b, "lat", across)
    far_a = lax.ppermute(buf_a, "lat", mates)

    local_sum, pert = pl.pallas_call(
        raise_kernel,
        name="raise",
        out_shape=[
            jax.ShapeDtypeStruct((ranks, part * band, lon), F32),
            jax.ShapeDtypeStruct((members, lev * band, lon), BF16),
        ],
        in_specs=[smem()] + [vmem()] * 2 + [anywhere()] * 4,
        out_specs=[vmem()] * 2,
        scratch_shapes=[
            pltpu.VMEM((3 * members * clev, clon), F32),
            pltpu.VMEM((lev * band, lon), F32),
            pltpu.VMEM((members, lev, band, lon), BF16),
            pltpu.VMEM((lev * band, lon), F32),
            pltpu.VMEM((members * clev, clon), F32),
            pltpu.VMEM(lon_up.shape, BF16),
            pltpu.VMEM(mix_up.shape, BF16),
            pltpu.SemaphoreType.DMA((members + 3,)),
        ],
        compiler_params=pltpu.CompilerParams(vmem_limit_bytes=VMEM_LIMIT),
    )(
        place, low_high[1], low_high[0],
        *[in_hbm(x) for x in (own, lon_up, mix_up, perturbations)],
    )
    parts = lax.all_to_all(local_sum, "mem", 0, 0, tiled=True)
    mine = call(total_kernel, "total", (band * part, lon), [(band * part * lon // 128, 128)], [], [parts])
    mate = lax.ppermute(mine, "lat", mates)
    pair = call(join_kernel, "join", (2 * band * part, lon), [], [], [mine, mate])
    far_pair = lax.ppermute(pair, "lat", far_chips)
    near_pair = lax.ppermute(pair, "lat", near_chips)

    n = rows + 2 * HALO
    north, east, west, weight = call(
        assemble_kernel, "assemble",
        [(n, 8, fine_lon), (n, 8, fine_lon), (n, 8, lon), (rows + 2 * PASSES, 8, fine_lon)],
        [], [place], [coef, own_weight, far_a, far_b],
    )
    piece = jax.ShapeDtypeStruct((band * part, lon), F32)
    keep, send_a, send_b = pl.pallas_call(
        fine_kernel,
        name="fine",
        out_shape=[piece] * 3,
        in_specs=[smem()] * 3 + [anywhere()] * 2 + [vmem()] * 8,
        out_specs=[vmem()] * 3,
        scratch_shapes=[
            pltpu.VMEM((5 * band, 8, lon), F32),
            pltpu.VMEM((n, 8, fine_lon), F32),
            pltpu.VMEM((3 * band, 8, lon), F32),
            pltpu.SMEM((1, 128), F32),
            pltpu.SMEM((1, 128), F32),
            pltpu.SemaphoreType.DMA((2,)),
        ],
        compiler_params=pltpu.CompilerParams(vmem_limit_bytes=VMEM_LIMIT),
    )(
        place, fine_source, fine_frac, far_a, far_b, mine, mate, near_pair, far_pair,
        north, east, west, weight,
    )
    got_b = lax.ppermute(send_b, "lat", across)
    got_a = lax.ppermute(send_a, "lat", mates)
    copies = call(
        copies_kernel, "copies", (ranks, band * part, lon),
        [(band * part * lon // 128, 128)], [], [keep, got_a, got_b]
    )
    adjoint = lax.all_to_all(copies, "mem", 0, 0, tiled=True)
    flat = (members * clev, clon)
    result, send_a, send_b = call(
        lower_kernel, "lower", [flat, flat, flat], [(3 * members * clev, lon)],
        [place], [own, pert, adjoint, mix_down, lon_down],
    )
    got_b = lax.ppermute(send_b, "lat", across)
    got_a = lax.ppermute(send_a, "lat", mates)
    return (result + got_a + got_b).reshape(controls.shape)


def solution(mesh):
    in_specs = (
        P("mem", None, "lat", None),
        P("mem", None, "lat", None),
        P(None, "lat", None),
        P("lat", None),
        P("lat", None),
        P("lat"),
        P("lat"),
    )
    out_specs = P("mem", None, "lat", None)
    return jax.shard_map(body, mesh=mesh, in_specs=in_specs, out_specs=out_specs, check_vma=False)
```

```python
import jax
import jax.numpy as jnp
import numpy as np
from jax import lax
from jax.experimental import pallas as pl
from jax.experimental.pallas import tpu as pltpu
from jax.sharding import PartitionSpec as P

PASSES = 5
REACH = 4
HALO = 2 * PASSES
VMEM_LIMIT = 24 * 2**20
F32 = jnp.float32
BF16 = jnp.bfloat16

PHASES = np.array(
    [[0.375, 0.625, 0.0], [0.125, 0.875, 0.0], [0.0, 0.875, 0.125], [0.0, 0.625, 0.375]]
)


def refine_matrix(count, periodic):
    matrix = np.zeros((4 * count, count), np.float32)
    for q in range(count):
        for r in range(4):
            for step in range(3):
                source = q + step - 1
                source = source % count if periodic else min(max(source, 0), count - 1)
                matrix[4 * q + r, source] += PHASES[r, step]
    return matrix


def split2(x):
    hi = x.astype(BF16)
    lo = (x - hi.astype(F32)).astype(BF16)
    return hi, lo


def position():
    lat = lax.axis_index("lat")
    return lat, lat % 2, lax.axis_size("lat") - 1


def dot(a, b):
    return jnp.dot(a, b, preferred_element_type=F32)


def prepare_kernel(
    source, frac, weight, north_all, east_all, select_all, order_all,
    coef, own_weight, buf_a, buf_b, level_weight, north, east, select, order, extra, sems,
):
    _, odd, _ = position()
    levels, rows, lon = level_weight.shape
    copies = [
        pltpu.make_async_copy(north_all, north, sems.at[0]),
        pltpu.make_async_copy(east_all, east, sems.at[1]),
        pltpu.make_async_copy(
            weight.at[pl.ds(lax.axis_index("mem") * levels, levels)], level_weight, sems.at[2]
        ),
        pltpu.make_async_copy(order_all, order, sems.at[3]),
        pltpu.make_async_copy(select_all, select, sems.at[4]),
    ]
    for copy in copies:
        copy.start()
    lane = lax.broadcasted_iota(jnp.int32, (4, 128), 1)
    tail = jnp.zeros((4, 128), F32)
    for k in range(rows):
        tail = jnp.where(lane == k, frac[k], tail)
        tail = jnp.where(lane == rows + k, source[k].astype(F32), tail)
    extra[...] = jnp.zeros(extra.shape, F32)
    extra[:, 0:128] = tail
    copies[0].wait()
    copies[1].wait()
    stacked = jnp.concatenate([north[...], east[...]], axis=0)
    hi = stacked.astype(BF16)
    rest = stacked - hi.astype(F32)
    mid = rest.astype(BF16)
    low = (rest - mid.astype(F32)).astype(BF16)
    copies[2].wait()
    copies[3].wait()
    values = dot(order[...], level_weight[...].reshape(levels * rows, lon)).astype(BF16)
    everything = jnp.concatenate([values, hi, mid, low], axis=0)
    copies[4].wait()
    many = levels * rows
    quarter = lon // 4
    for c in range(lon // 512):
        moved = dot(everything[:, 512 * c : 512 * c + 512], select[...])
        wpart = moved[:many]
        cpart = moved[many : many + 2 * rows] + moved[many + 2 * rows : many + 4 * rows]
        cpart = cpart + moved[many + 4 * rows :]
        for r in range(4):
            to = slice(quarter * r + 128 * c, quarter * r + 128 * c + 128)
            frm = slice(128 * r, 128 * r + 128)
            coef[:, to] = cpart[:, frm]
            own_weight[:, :, to] = wpart[:, frm].reshape(rows, levels, 128).astype(BF16)

    def fill(buf, upper):
        first = rows - PASSES if upper else 0
        for k in range(PASSES):
            buf[8 * k : 8 * k + 8, :] = own_weight[first + k].astype(F32)
        first = rows - HALO if upper else 0
        base = 8 * PASSES
        buf[base : base + HALO, :] = coef[first : first + HALO, :]
        buf[base + HALO : base + 2 * HALO, :] = coef[rows + first : rows + first + HALO, :]
        buf[base + 2 * HALO :, :] = extra[...]

    @pl.when(odd == 0)
    def _():
        fill(buf_a, True)
        fill(buf_b, False)

    @pl.when(odd == 1)
    def _():
        fill(buf_a, False)
        fill(buf_b, True)


def assemble_kernel(coef, own_weight, got_a, got_b, north, east, west, weight):
    lat, odd, _ = position()
    rows = own_weight.shape[0]
    quarter = coef.shape[1] // 4

    def put(i, nrow, erow):
        shape = (8, coef.shape[1])
        north[i] = jnp.broadcast_to(nrow, shape)
        spread = jnp.broadcast_to(erow, shape)
        east[i] = spread
        west[i] = pltpu.roll(spread[:, 3 * quarter :], 1, axis=1)

    for k in range(rows):
        put(HALO + k, coef[k : k + 1, :], coef[rows + k : rows + k + 1, :])
        weight[PASSES + k] = own_weight[k].astype(F32)

    def side(buf, start, wstart):
        base = 8 * PASSES
        for k in range(HALO):
            put(start + k, buf[base + k : base + k + 1, :], buf[base + HALO + k : base + HALO + k + 1, :])
        for k in range(PASSES):
            weight[wstart + k] = buf[8 * k : 8 * k + 8, :]

    @pl.when(odd == 0)
    def _():
        side(got_b, 0, 0)
        side(got_a, HALO + rows, PASSES + rows)

    @pl.when(odd == 1)
    def _():
        side(got_a, 0, 0)
        side(got_b, HALO + rows, PASSES + rows)

    @pl.when(lat == 0)
    def _():
        north[HALO - 1] = jnp.zeros(north.shape[1:], F32)


def arrange_kernel(own_all, lon_all, mix_all, stored, own, lon_up, mix, pert, raw, flat, sems):
    members, levels, band, _ = raw.shape
    small = [
        pltpu.make_async_copy(own_all, own, sems.at[members]),
        pltpu.make_async_copy(lon_all, lon_up, sems.at[members + 1]),
        pltpu.make_async_copy(mix_all, mix, sems.at[members + 2]),
    ]
    copies = [pltpu.make_async_copy(stored.at[m], raw.at[m], sems.at[m]) for m in range(members)]
    for copy in copies + small:
        copy.start()
    for m in range(members):
        copies[m].wait()
        values = raw[m].astype(F32)
        for k in range(levels):
            flat[m, band * k : band * k + band, :] = values[k]
        pert[m] = flat[m].astype(BF16)
    for copy in small:
        copy.wait()


def raise_kernel(got_a, got_b, own, lon_up, mix, pert, out, x, acc):
    lat, odd, last = position()
    members = pert.shape[0]
    lev = own.shape[0] // members

    def put(step, ref):
        for m in range(members):
            at = (3 * m + step) * lev
            x[at : at + lev, :] = ref[m * lev : m * lev + lev, :]

    put(1, own)

    @pl.when(lat == 0)
    def _():
        put(0, own)

    @pl.when((lat > 0) & (odd == 0))
    def _():
        put(0, got_b)

    @pl.when(odd == 1)
    def _():
        put(0, got_a)

    @pl.when(lat == last)
    def _():
        put(2, own)

    @pl.when((lat < last) & (odd == 1))
    def _():
        put(2, got_b)

    @pl.when(odd == 0)
    def _():
        put(2, got_a)

    hi, lo = split2(x[...])
    wide = dot(hi, lon_up[...]) + dot(lo, lon_up[...])
    for m in range(members):
        hi, lo = split2(wide[3 * lev * m : 3 * lev * (m + 1), :])
        field = dot(mix[...], jnp.concatenate([hi, lo], axis=0))
        term = field * pert[m].astype(F32)
        if m == 0:
            acc[...] = term
        elif m < members - 1:
            acc[...] += term
        else:
            out[...] = (acc[...] + term).reshape(out.shape)


def total_kernel(parts, out, sums):
    count, n, lon = parts.shape
    total = parts[0]
    for k in range(1, count):
        total = total + parts[k]
    rows = n // 8
    for c in range(lon // 128):
        lanes = slice(128 * c, 128 * c + 128)
        sums[n * c : n * c + n, :] = total[:, lanes]
        for row in range(rows):
            out[8 * row : 8 * row + 8, lanes] = sums[pl.ds(n * c + row, 8, stride=rows), :]


def join_kernel(mine, mate, out):
    half = mine.shape[0]
    out[:half] = mine[...]
    out[half:] = mate[...]


def fine_kernel(
    source_all, frac_all, far_a, far_b, own, mate, near_pair, far_pair,
    north, east, west, weight, keep, send_a, send_b, mid, v, acc, extra_a, extra_b, source, frac, sems,
):
    at = 8 * PASSES + 2 * HALO
    copies = [
        pltpu.make_async_copy(far_a.at[at : at + 1, 0:128], extra_a, sems.at[0]),
        pltpu.make_async_copy(far_b.at[at : at + 1, 0:128], extra_b, sems.at[1]),
        pltpu.make_async_copy(source_all, source, sems.at[2]),
        pltpu.make_async_copy(frac_all, frac, sems.at[3]),
    ]
    for copy in copies:
        copy.start()
    lat, odd, last = position()
    lon = own.shape[1]
    rows = source.shape[0]
    n = rows + 2 * HALO
    band = own.shape[0] // 8

    def bring(slot, ref, start):
        for k in range(band):
            mid[slot * band + k] = ref[start + 8 * k : start + 8 * k + 8, :]

    half = own.shape[0]
    bring(2, own, 0)

    def gather(even, up_pair, down_pair):
        bring(0, up_pair, 0)
        bring(4, down_pair, 0)
        if even:
            bring(1, up_pair, half)
            bring(3, mate, 0)
        else:
            bring(1, mate, 0)
            bring(3, down_pair, half)

    turn = lat % 4
    for case in range(4):

        @pl.when(turn == case)
        def _(case=case):
            if case < 2:
                gather(case % 2 == 0, far_pair, near_pair)
            else:
                gather(case % 2 == 0, near_pair, far_pair)

    copies[2].wait()
    copies[3].wait()
    origin = (lat - 2) * band
    inner = list(range(HALO, HALO + rows))
    for i in inner + [i for i in range(n) if i not in inner]:
        if i == 0:
            copies[0].wait()
            copies[1].wait()
        k = i - HALO
        if k < 0:
            k += rows
            f = jnp.where(odd == 1, extra_a[0, k], extra_b[0, k])
            s = jnp.where(odd == 1, extra_a[0, rows + k], extra_b[0, rows + k]).astype(jnp.int32)
            valid = jnp.where(lat > 0, 1.0, 0.0)
        elif k >= rows:
            k -= rows
            f = jnp.where(odd == 0, extra_a[0, k], extra_b[0, k])
            s = jnp.where(odd == 0, extra_a[0, rows + k], extra_b[0, rows + k]).astype(jnp.int32)
            valid = jnp.where(lat < last, 1.0, 0.0)
        else:
            f, s, valid = frac[k], source[k], None
        s = jnp.clip(s - origin, 0, 5 * band - 2)
        below, above = 1.0 - f, f
        if valid is not None:
            below, above = below * valid, above * valid
        cur = below * mid[s] + above * mid[s + 1]
        prev = pltpu.roll(cur, 1, axis=1)
        nxt = pltpu.roll(cur, lon - 1, axis=1)
        v[i, :, 0:lon] = 0.375 * prev + 0.625 * cur
        v[i, :, lon : 2 * lon] = 0.125 * prev + 0.875 * cur
        v[i, :, 2 * lon : 3 * lon] = 0.875 * cur + 0.125 * nxt
        v[i, :, 3 * lon : 4 * lon] = 0.625 * cur + 0.375 * nxt

    inside_top = jnp.where(lat < last, 1.0, 0.0)

    def cut(r):
        return slice(r * lon, r * lon + lon)

    def sweep(first, stop, finish):
        def flux(i, here, there):
            return [north[i, :, cut(r)] * (there[r] - here[r]) for r in range(4)]

        before = [v[first - 1, :, cut(r)] for r in range(4)]
        here = [v[first, :, cut(r)] for r in range(4)]
        low = flux(first - 1, before, here)
        for i in range(first, stop):
            there = [v[i + 1, :, cut(r)] for r in range(4)]
            high = flux(i, here, there)
            if i == HALO + rows:
                low = [inside_top * x for x in low]
            right = pltpu.roll(here[0], lon - 1, axis=1)
            left = pltpu.roll(here[3], 1, axis=1)
            side = [
                east[i, :, cut(r)] * ((here[r + 1] if r < 3 else right) - here[r]) for r in range(4)
            ]
            back = [west[i] * (here[0] - left)] + side[:3]
            new = [here[r] + ((high[r] - low[r]) + (side[r] - back[r])) for r in range(4)]
            finish(i, new)
            low, here = high, there

    def store(i, new):
        for r in range(4):
            v[i, :, cut(r)] = new[r]

    def store_weighted(i, new):
        for r in range(4):
            v[i, :, cut(r)] = weight[i - PASSES, :, cut(r)] * new[r]

    acc[...] = jnp.zeros(acc.shape, F32)
    base = (lat - 1) * band

    def spread(i, o):
        k = i - HALO
        ahead = pltpu.roll(0.375 * o[0] + 0.125 * o[1], lon - 1, axis=1)
        behind = pltpu.roll(0.125 * o[2] + 0.375 * o[3], 1, axis=1)
        g = 0.625 * (o[0] + o[3]) + 0.875 * (o[1] + o[2]) + (ahead + behind)
        s = jnp.clip(source[k] - base, 0, 3 * band - 2)
        f = frac[k]
        acc[s] += (1.0 - f) * g
        acc[s + 1] += f * g

    def first_pass(_, carry):
        sweep(1, n - 1, store)
        return carry

    def second_pass(_, carry):
        sweep(PASSES + 1, n - PASSES - 1, store)
        return carry

    lax.fori_loop(0, PASSES - 1, first_pass, 0)
    sweep(PASSES, n - PASSES, store_weighted)
    lax.fori_loop(0, PASSES - 1, second_pass, 0)
    sweep(HALO, HALO + rows, spread)
    for k in range(band):
        keep[8 * k : 8 * k + 8, :] = acc[band + k]

    def give(ref, slot):
        for k in range(band):
            ref[8 * k : 8 * k + 8, :] = acc[slot * band + k]

    @pl.when(odd == 0)
    def _():
        give(send_a, 2)
        give(send_b, 0)

    @pl.when(odd == 1)
    def _():
        give(send_a, 0)
        give(send_b, 2)


def copies_kernel(keep, got_a, got_b, out, sums):
    count, n, lon = out.shape
    rows = n // 8
    total = keep[...] + got_a[...] + got_b[...]
    for c in range(lon // 128):
        lanes = slice(128 * c, 128 * c + 128)
        for row in range(rows):
            sums[pl.ds(n * c + row, 8, stride=rows), :] = total[8 * row : 8 * row + 8, lanes]
        value = sums[n * c : n * c + n, :]
        for k in range(count):
            out[k, :, lanes] = value


def lower_kernel(controls, pert, adjoint, mix_t, lon_down, own, send_a, send_b, wide):
    lat, odd, last = position()
    members = pert.shape[0]
    lev = own.shape[0] // members
    field = adjoint[...].reshape(pert.shape[1], pert.shape[2])
    for m in range(members):
        hi, lo = split2(field * pert[m].astype(F32))
        wide[3 * lev * m : 3 * lev * (m + 1), :] = dot(mix_t[...], hi) + dot(mix_t[...], lo)
    hi, lo = split2(wide[...])
    narrow = dot(hi, lon_down[...]) + dot(lo, lon_down[...])
    at_first = jnp.where(lat == 0, 1.0, 0.0)
    at_last = jnp.where(lat == last, 1.0, 0.0)
    is_odd = jnp.where(odd == 1, 1.0, 0.0)
    for m in range(members):
        at = 3 * lev * m
        low = narrow[at : at + lev]
        mine = narrow[at + lev : at + 2 * lev]
        high = narrow[at + 2 * lev : at + 3 * lev]
        to = slice(m * lev, m * lev + lev)
        own[to, :] = controls[to, :] + mine + at_first * low + at_last * high
        low = (1.0 - at_first) * low
        high = (1.0 - at_last) * high
        send_a[to, :] = is_odd * low + (1.0 - is_odd) * high
        send_b[to, :] = is_odd * high + (1.0 - is_odd) * low


def vmem():
    return pl.BlockSpec(memory_space=pltpu.VMEM)


def anywhere():
    return pl.BlockSpec(memory_space=pl.ANY)


def in_hbm(x):
    return pltpu.with_memory_space_constraint(x, pltpu.HBM)


def smem():
    return pl.BlockSpec(memory_space=pltpu.SMEM)


def call(kernel, name, outs, scratch, scalars, vectors):
    many = isinstance(outs, list)
    shapes = [jax.ShapeDtypeStruct(s, F32) for s in (outs if many else [outs])]
    return pl.pallas_call(
        kernel,
        name=name,
        out_shape=shapes if many else shapes[0],
        in_specs=[smem()] * len(scalars) + [vmem()] * len(vectors),
        out_specs=[vmem()] * len(shapes) if many else vmem(),
        scratch_shapes=[pltpu.VMEM(s, F32) for s in scratch],
        compiler_params=pltpu.CompilerParams(vmem_limit_bytes=VMEM_LIMIT),
    )(*scalars, *vectors)


def body(controls, perturbations, precision_weight, north_coef, east_coef, fine_source, fine_frac):
    count = lax.axis_size("lat")
    ranks = lax.axis_size("mem")
    members, clev, _, clon = controls.shape
    lev, band, lon = perturbations.shape[1:]
    rows, fine_lon = north_coef.shape
    part = lev // ranks

    mates = [(i, i ^ 1) for i in range(count)]
    across = [(i, (i + 1) % count if i % 2 else (i - 1) % count) for i in range(count)]
    near_chips = [(i, i ^ 2) for i in range(count)]
    far_chips = [(i, (i + 2) % count if i & 2 else (i - 2) % count) for i in range(count)]

    lon_refine = refine_matrix(clon, True)
    lev_refine = refine_matrix(clev, False)
    mix = np.einsum("vl,rt->vrtl", lev_refine, PHASES).reshape(lev * band, 3 * clev)
    lon_up = jnp.asarray(lon_refine.T, BF16)
    lon_down = jnp.asarray(lon_refine, BF16)
    mix_up = jnp.asarray(np.concatenate([mix, mix], axis=1), BF16)
    mix_down = jnp.asarray(mix.T, BF16)
    pick = np.zeros((512, 512), np.float32)
    for r in range(4):
        for q in range(128):
            pick[4 * q + r, 128 * r + q] = 1.0
    pick = jnp.asarray(pick, BF16)
    order = np.eye(part * rows).reshape(part, rows, part, rows).transpose(1, 0, 2, 3)
    order = jnp.asarray(order.reshape(part * rows, part * rows), BF16)

    own = controls.reshape(members * clev, clon)
    low_high = [lax.ppermute(own, "lat", across), lax.ppermute(own, "lat", mates)]

    spots = 8 * PASSES + 2 * HALO + 4
    coef, own_weight, buf_a, buf_b = pl.pallas_call(
        prepare_kernel,
        name="prepare",
        out_shape=[
            jax.ShapeDtypeStruct((2 * rows, fine_lon), F32),
            jax.ShapeDtypeStruct((rows, part, fine_lon), BF16),
            jax.ShapeDtypeStruct((spots, fine_lon), F32),
            jax.ShapeDtypeStruct((spots, fine_lon), F32),
        ],
        in_specs=[smem()] * 2 + [anywhere()] * 5,
        out_specs=[vmem()] * 4,
        scratch_shapes=[
            pltpu.VMEM((part, rows, fine_lon), BF16),
            pltpu.VMEM((rows, fine_lon), F32),
            pltpu.VMEM((rows, fine_lon), F32),
            pltpu.VMEM((512, 512), BF16),
            pltpu.VMEM((part * rows, part * rows), BF16),
            pltpu.VMEM((4, fine_lon), F32),
            pltpu.SemaphoreType.DMA((5,)),
        ],
        compiler_params=pltpu.CompilerParams(vmem_limit_bytes=VMEM_LIMIT),
    )(
        fine_source, fine_frac,
        *[in_hbm(x) for x in (precision_weight, north_coef, east_coef, pick, order)],
    )
    far_b = lax.ppermute(buf_b, "lat", across)
    far_a = lax.ppermute(buf_a, "lat", mates)

    flat_shape = (members * clev, clon)
    own_copy, lon_copy, mix_copy, pert = pl.pallas_call(
        arrange_kernel,
        name="arrange",
        out_shape=[
            jax.ShapeDtypeStruct(flat_shape, F32),
            jax.ShapeDtypeStruct(lon_up.shape, BF16),
            jax.ShapeDtypeStruct(mix_up.shape, BF16),
            jax.ShapeDtypeStruct((members, lev * band, lon), BF16),
        ],
        in_specs=[anywhere()] * 4,
        out_specs=[vmem()] * 4,
        scratch_shapes=[
            pltpu.VMEM((members, lev, band, lon), BF16),
            pltpu.VMEM((members, lev * band, lon), F32),
            pltpu.SemaphoreType.DMA((members + 3,)),
        ],
        compiler_params=pltpu.CompilerParams(vmem_limit_bytes=VMEM_LIMIT),
    )(*[in_hbm(x) for x in (own, lon_up, mix_up, perturbations)])
    local_sum = call(
        raise_kernel, "raise", (ranks, part * band, lon),
        [(3 * members * clev, clon), (lev * band, lon)],
        [], [low_high[1], low_high[0], own_copy, lon_copy, mix_copy, pert],
    )
    parts = lax.all_to_all(local_sum, "mem", 0, 0, tiled=True)
    mine = call(total_kernel, "total", (band * part, lon), [(band * part * lon // 128, 128)], [], [parts])
    mate = lax.ppermute(mine, "lat", mates)
    pair = call(join_kernel, "join", (2 * band * part, lon), [], [], [mine, mate])
    far_pair = lax.ppermute(pair, "lat", far_chips)
    near_pair = lax.ppermute(pair, "lat", near_chips)

    n = rows + 2 * HALO
    north, east, west, weight = call(
        assemble_kernel, "assemble",
        [(n, 8, fine_lon), (n, 8, fine_lon), (n, 8, lon), (rows + 2 * PASSES, 8, fine_lon)],
        [], [], [coef, own_weight, far_a, far_b],
    )
    piece = jax.ShapeDtypeStruct((band * part, lon), F32)
    keep, send_a, send_b = pl.pallas_call(
        fine_kernel,
        name="fine",
        out_shape=[piece] * 3,
        in_specs=[anywhere()] * 4 + [vmem()] * 8,
        out_specs=[vmem()] * 3,
        scratch_shapes=[
            pltpu.VMEM((5 * band, 8, lon), F32),
            pltpu.VMEM((n, 8, fine_lon), F32),
            pltpu.VMEM((3 * band, 8, lon), F32),
            pltpu.SMEM((1, 128), F32),
            pltpu.SMEM((1, 128), F32),
            pltpu.SMEM((rows,), jnp.int32),
            pltpu.SMEM((rows,), F32),
            pltpu.SemaphoreType.DMA((4,)),
        ],
        compiler_params=pltpu.CompilerParams(vmem_limit_bytes=VMEM_LIMIT),
    )(
        fine_source, fine_frac, far_a, far_b, mine, mate, near_pair, far_pair,
        north, east, west, weight,
    )
    got_b = lax.ppermute(send_b, "lat", across)
    got_a = lax.ppermute(send_a, "lat", mates)
    copies = call(
        copies_kernel, "copies", (ranks, band * part, lon),
        [(band * part * lon // 128, 128)], [], [keep, got_a, got_b]
    )
    adjoint = lax.all_to_all(copies, "mem", 0, 0, tiled=True)
    flat = (members * clev, clon)
    result, send_a, send_b = call(
        lower_kernel, "lower", [flat, flat, flat], [(3 * members * clev, lon)],
        [], [own, pert, adjoint, mix_down, lon_down],
    )
    got_b = lax.ppermute(send_b, "lat", across)
    got_a = lax.ppermute(send_a, "lat", mates)
    return (result + got_a + got_b).reshape(controls.shape)


def solution(mesh):
    in_specs = (
        P("mem", None, "lat", None),
        P("mem", None, "lat", None),
        P(None, "lat", None),
        P("lat", None),
        P("lat", None),
        P("lat"),
        P("lat"),
    )
    out_specs = P("mem", None, "lat", None)
    return jax.shard_map(body, mesh=mesh, in_specs=in_specs, out_specs=out_specs, check_vma=False)
```

```python
import jax
import jax.numpy as jnp
import numpy as np
from jax import lax
from jax.experimental import pallas as pl
from jax.experimental.pallas import tpu as pltpu
from jax.sharding import PartitionSpec as P

PASSES = 5
REACH = 4
HALO = 2 * PASSES
VMEM_LIMIT = 24 * 2**20
F32 = jnp.float32
BF16 = jnp.bfloat16

PHASES = np.array(
    [[0.375, 0.625, 0.0], [0.125, 0.875, 0.0], [0.0, 0.875, 0.125], [0.0, 0.625, 0.375]]
)


def refine_matrix(count, periodic):
    matrix = np.zeros((4 * count, count), np.float32)
    for q in range(count):
        for r in range(4):
            for step in range(3):
                source = q + step - 1
                source = source % count if periodic else min(max(source, 0), count - 1)
                matrix[4 * q + r, source] += PHASES[r, step]
    return matrix


def split2(x):
    hi = x.astype(BF16)
    lo = (x - hi.astype(F32)).astype(BF16)
    return hi, lo


def position():
    lat = lax.axis_index("lat")
    return lat, lat % 2, lax.axis_size("lat") - 1


def dot(a, b):
    return jnp.dot(a, b, preferred_element_type=F32)


def prepare_kernel(
    source, frac, level_weight, north, east, select, order,
    coef, own_weight, buf_a, buf_b, extra,
):
    _, odd, _ = position()
    levels, rows, lon = level_weight.shape
    lane = lax.broadcasted_iota(jnp.int32, (4, 128), 1)
    tail = jnp.zeros((4, 128), F32)
    for k in range(rows):
        tail = jnp.where(lane == k, frac[k], tail)
        tail = jnp.where(lane == rows + k, source[k].astype(F32), tail)
    extra[...] = jnp.zeros(extra.shape, F32)
    extra[:, 0:128] = tail
    stacked = jnp.concatenate([north[...], east[...]], axis=0)
    hi = stacked.astype(BF16)
    rest = stacked - hi.astype(F32)
    mid = rest.astype(BF16)
    low = (rest - mid.astype(F32)).astype(BF16)
    values = dot(order[...], level_weight[...].reshape(levels * rows, lon)).astype(BF16)
    everything = jnp.concatenate([values, hi, mid, low], axis=0)
    many = levels * rows
    quarter = lon // 4
    for c in range(lon // 512):
        moved = dot(everything[:, 512 * c : 512 * c + 512], select[...])
        wpart = moved[:many]
        cpart = moved[many : many + 2 * rows] + moved[many + 2 * rows : many + 4 * rows]
        cpart = cpart + moved[many + 4 * rows :]
        for r in range(4):
            to = slice(quarter * r + 128 * c, quarter * r + 128 * c + 128)
            frm = slice(128 * r, 128 * r + 128)
            coef[:, to] = cpart[:, frm]
            own_weight[:, :, to] = wpart[:, frm].reshape(rows, levels, 128).astype(BF16)

    def fill(buf, upper):
        first = rows - PASSES if upper else 0
        for k in range(PASSES):
            buf[8 * k : 8 * k + 8, :] = own_weight[first + k].astype(F32)
        first = rows - HALO if upper else 0
        base = 8 * PASSES
        buf[base : base + HALO, :] = coef[first : first + HALO, :]
        buf[base + HALO : base + 2 * HALO, :] = coef[rows + first : rows + first + HALO, :]
        buf[base + 2 * HALO :, :] = extra[...]

    @pl.when(odd == 0)
    def _():
        fill(buf_a, True)
        fill(buf_b, False)

    @pl.when(odd == 1)
    def _():
        fill(buf_a, False)
        fill(buf_b, True)


def assemble_kernel(coef, own_weight, got_a, got_b, north, east, west, weight):
    lat, odd, _ = position()
    rows = own_weight.shape[0]
    quarter = coef.shape[1] // 4

    def put(i, nrow, erow):
        shape = (8, coef.shape[1])
        north[i] = jnp.broadcast_to(nrow, shape)
        spread = jnp.broadcast_to(erow, shape)
        east[i] = spread
        west[i] = pltpu.roll(spread[:, 3 * quarter :], 1, axis=1)

    for k in range(rows):
        put(HALO + k, coef[k : k + 1, :], coef[rows + k : rows + k + 1, :])
        weight[PASSES + k] = own_weight[k].astype(F32)

    def side(buf, start, wstart):
        base = 8 * PASSES
        for k in range(HALO):
            put(start + k, buf[base + k : base + k + 1, :], buf[base + HALO + k : base + HALO + k + 1, :])
        for k in range(PASSES):
            weight[wstart + k] = buf[8 * k : 8 * k + 8, :]

    @pl.when(odd == 0)
    def _():
        side(got_b, 0, 0)
        side(got_a, HALO + rows, PASSES + rows)

    @pl.when(odd == 1)
    def _():
        side(got_a, 0, 0)
        side(got_b, HALO + rows, PASSES + rows)

    @pl.when(lat == 0)
    def _():
        north[HALO - 1] = jnp.zeros(north.shape[1:], F32)


def arrange_kernel(
    own_all, lon_all, mix_all, stored, weight_all, north_all, east_all, select_all, order_all,
    own, lon_up, mix, pert, weight, north, east, select, order, raw, flat, sems,
):
    members, levels, band, _ = raw.shape
    small = [
        pltpu.make_async_copy(own_all, own, sems.at[members]),
        pltpu.make_async_copy(lon_all, lon_up, sems.at[members + 1]),
        pltpu.make_async_copy(mix_all, mix, sems.at[members + 2]),
    ]
    copies = [pltpu.make_async_copy(stored.at[m], raw.at[m], sems.at[m]) for m in range(members)]
    levels_here = weight_all.at[pl.ds(lax.axis_index("mem") * weight.shape[0], weight.shape[0])]
    small += [
        pltpu.make_async_copy(levels_here, weight, sems.at[members + 3]),
        pltpu.make_async_copy(north_all, north, sems.at[members + 4]),
        pltpu.make_async_copy(east_all, east, sems.at[members + 5]),
        pltpu.make_async_copy(select_all, select, sems.at[members + 6]),
        pltpu.make_async_copy(order_all, order, sems.at[members + 7]),
    ]
    for copy in copies + small:
        copy.start()
    for m in range(members):
        copies[m].wait()
        values = raw[m].astype(F32)
        for k in range(levels):
            flat[m, band * k : band * k + band, :] = values[k]
        pert[m] = flat[m].astype(BF16)
    for copy in small:
        copy.wait()


def raise_kernel(got_a, got_b, own, lon_up, mix, pert, out, x, acc):
    lat, odd, last = position()
    members = pert.shape[0]
    lev = own.shape[0] // members

    def put(step, ref):
        for m in range(members):
            at = (3 * m + step) * lev
            x[at : at + lev, :] = ref[m * lev : m * lev + lev, :]

    put(1, own)

    @pl.when(lat == 0)
    def _():
        put(0, own)

    @pl.when((lat > 0) & (odd == 0))
    def _():
        put(0, got_b)

    @pl.when(odd == 1)
    def _():
        put(0, got_a)

    @pl.when(lat == last)
    def _():
        put(2, own)

    @pl.when((lat < last) & (odd == 1))
    def _():
        put(2, got_b)

    @pl.when(odd == 0)
    def _():
        put(2, got_a)

    hi, lo = split2(x[...])
    wide = dot(hi, lon_up[...]) + dot(lo, lon_up[...])
    for m in range(members):
        hi, lo = split2(wide[3 * lev * m : 3 * lev * (m + 1), :])
        field = dot(mix[...], jnp.concatenate([hi, lo], axis=0))
        term = field * pert[m].astype(F32)
        if m == 0:
            acc[...] = term
        elif m < members - 1:
            acc[...] += term
        else:
            out[...] = (acc[...] + term).reshape(out.shape)


def total_kernel(parts, out, sums):
    count, n, lon = parts.shape
    total = parts[0]
    for k in range(1, count):
        total = total + parts[k]
    rows = n // 8
    for c in range(lon // 128):
        lanes = slice(128 * c, 128 * c + 128)
        sums[n * c : n * c + n, :] = total[:, lanes]
        for row in range(rows):
            out[8 * row : 8 * row + 8, lanes] = sums[pl.ds(n * c + row, 8, stride=rows), :]


def join_kernel(mine, mate, out):
    half = mine.shape[0]
    out[:half] = mine[...]
    out[half:] = mate[...]


def fine_kernel(
    source_all, frac_all, far_a, far_b, own, mate, near_pair, far_pair,
    north, east, west, weight, keep, send_a, send_b, mid, v, acc, extra_a, extra_b, source, frac, sems,
):
    at = 8 * PASSES + 2 * HALO
    copies = [
        pltpu.make_async_copy(far_a.at[at : at + 1, 0:128], extra_a, sems.at[0]),
        pltpu.make_async_copy(far_b.at[at : at + 1, 0:128], extra_b, sems.at[1]),
        pltpu.make_async_copy(source_all, source, sems.at[2]),
        pltpu.make_async_copy(frac_all, frac, sems.at[3]),
    ]
    for copy in copies:
        copy.start()
    lat, odd, last = position()
    lon = own.shape[1]
    rows = source.shape[0]
    n = rows + 2 * HALO
    band = own.shape[0] // 8

    def bring(slot, ref, start):
        for k in range(band):
            mid[slot * band + k] = ref[start + 8 * k : start + 8 * k + 8, :]

    half = own.shape[0]
    bring(2, own, 0)

    def gather(even, up_pair, down_pair):
        bring(0, up_pair, 0)
        bring(4, down_pair, 0)
        if even:
            bring(1, up_pair, half)
            bring(3, mate, 0)
        else:
            bring(1, mate, 0)
            bring(3, down_pair, half)

    turn = lat % 4
    for case in range(4):

        @pl.when(turn == case)
        def _(case=case):
            if case < 2:
                gather(case % 2 == 0, far_pair, near_pair)
            else:
                gather(case % 2 == 0, near_pair, far_pair)

    copies[2].wait()
    copies[3].wait()
    origin = (lat - 2) * band
    inner = list(range(HALO, HALO + rows))
    for i in inner + [i for i in range(n) if i not in inner]:
        if i == 0:
            copies[0].wait()
            copies[1].wait()
        k = i - HALO
        if k < 0:
            k += rows
            f = jnp.where(odd == 1, extra_a[0, k], extra_b[0, k])
            s = jnp.where(odd == 1, extra_a[0, rows + k], extra_b[0, rows + k]).astype(jnp.int32)
            valid = jnp.where(lat > 0, 1.0, 0.0)
        elif k >= rows:
            k -= rows
            f = jnp.where(odd == 0, extra_a[0, k], extra_b[0, k])
            s = jnp.where(odd == 0, extra_a[0, rows + k], extra_b[0, rows + k]).astype(jnp.int32)
            valid = jnp.where(lat < last, 1.0, 0.0)
        else:
            f, s, valid = frac[k], source[k], None
        s = jnp.clip(s - origin, 0, 5 * band - 2)
        below, above = 1.0 - f, f
        if valid is not None:
            below, above = below * valid, above * valid
        cur = below * mid[s] + above * mid[s + 1]
        prev = pltpu.roll(cur, 1, axis=1)
        nxt = pltpu.roll(cur, lon - 1, axis=1)
        v[i, :, 0:lon] = 0.375 * prev + 0.625 * cur
        v[i, :, lon : 2 * lon] = 0.125 * prev + 0.875 * cur
        v[i, :, 2 * lon : 3 * lon] = 0.875 * cur + 0.125 * nxt
        v[i, :, 3 * lon : 4 * lon] = 0.625 * cur + 0.375 * nxt

    inside_top = jnp.where(lat < last, 1.0, 0.0)

    def cut(r):
        return slice(r * lon, r * lon + lon)

    def sweep(first, stop, finish):
        def flux(i, here, there):
            return [north[i, :, cut(r)] * (there[r] - here[r]) for r in range(4)]

        before = [v[first - 1, :, cut(r)] for r in range(4)]
        here = [v[first, :, cut(r)] for r in range(4)]
        low = flux(first - 1, before, here)
        for i in range(first, stop):
            there = [v[i + 1, :, cut(r)] for r in range(4)]
            high = flux(i, here, there)
            if i == HALO + rows:
                low = [inside_top * x for x in low]
            right = pltpu.roll(here[0], lon - 1, axis=1)
            left = pltpu.roll(here[3], 1, axis=1)
            side = [
                east[i, :, cut(r)] * ((here[r + 1] if r < 3 else right) - here[r]) for r in range(4)
            ]
            back = [west[i] * (here[0] - left)] + side[:3]
            new = [here[r] + ((high[r] - low[r]) + (side[r] - back[r])) for r in range(4)]
            finish(i, new)
            low, here = high, there

    def store(i, new):
        for r in range(4):
            v[i, :, cut(r)] = new[r]

    def store_weighted(i, new):
        for r in range(4):
            v[i, :, cut(r)] = weight[i - PASSES, :, cut(r)] * new[r]

    acc[...] = jnp.zeros(acc.shape, F32)
    base = (lat - 1) * band

    def spread(i, o):
        k = i - HALO
        ahead = pltpu.roll(0.375 * o[0] + 0.125 * o[1], lon - 1, axis=1)
        behind = pltpu.roll(0.125 * o[2] + 0.375 * o[3], 1, axis=1)
        g = 0.625 * (o[0] + o[3]) + 0.875 * (o[1] + o[2]) + (ahead + behind)
        s = jnp.clip(source[k] - base, 0, 3 * band - 2)
        f = frac[k]
        acc[s] += (1.0 - f) * g
        acc[s + 1] += f * g

    def first_pass(_, carry):
        sweep(1, n - 1, store)
        return carry

    def second_pass(_, carry):
        sweep(PASSES + 1, n - PASSES - 1, store)
        return carry

    lax.fori_loop(0, PASSES - 1, first_pass, 0)
    sweep(PASSES, n - PASSES, store_weighted)
    lax.fori_loop(0, PASSES - 1, second_pass, 0)
    sweep(HALO, HALO + rows, spread)
    for k in range(band):
        keep[8 * k : 8 * k + 8, :] = acc[band + k]

    def give(ref, slot):
        for k in range(band):
            ref[8 * k : 8 * k + 8, :] = acc[slot * band + k]

    @pl.when(odd == 0)
    def _():
        give(send_a, 2)
        give(send_b, 0)

    @pl.when(odd == 1)
    def _():
        give(send_a, 0)
        give(send_b, 2)


def copies_kernel(keep, got_a, got_b, out, sums):
    count, n, lon = out.shape
    rows = n // 8
    total = keep[...] + got_a[...] + got_b[...]
    for c in range(lon // 128):
        lanes = slice(128 * c, 128 * c + 128)
        for row in range(rows):
            sums[pl.ds(n * c + row, 8, stride=rows), :] = total[8 * row : 8 * row + 8, lanes]
        value = sums[n * c : n * c + n, :]
        for k in range(count):
            out[k, :, lanes] = value


def lower_kernel(controls, pert, adjoint, mix_t, lon_down, own, send_a, send_b, wide):
    lat, odd, last = position()
    members = pert.shape[0]
    lev = own.shape[0] // members
    field = adjoint[...].reshape(pert.shape[1], pert.shape[2])
    for m in range(members):
        hi, lo = split2(field * pert[m].astype(F32))
        wide[3 * lev * m : 3 * lev * (m + 1), :] = dot(mix_t[...], hi) + dot(mix_t[...], lo)
    hi, lo = split2(wide[...])
    narrow = dot(hi, lon_down[...]) + dot(lo, lon_down[...])
    at_first = jnp.where(lat == 0, 1.0, 0.0)
    at_last = jnp.where(lat == last, 1.0, 0.0)
    is_odd = jnp.where(odd == 1, 1.0, 0.0)
    for m in range(members):
        at = 3 * lev * m
        low = narrow[at : at + lev]
        mine = narrow[at + lev : at + 2 * lev]
        high = narrow[at + 2 * lev : at + 3 * lev]
        to = slice(m * lev, m * lev + lev)
        own[to, :] = controls[to, :] + mine + at_first * low + at_last * high
        low = (1.0 - at_first) * low
        high = (1.0 - at_last) * high
        send_a[to, :] = is_odd * low + (1.0 - is_odd) * high
        send_b[to, :] = is_odd * high + (1.0 - is_odd) * low


def vmem():
    return pl.BlockSpec(memory_space=pltpu.VMEM)


def anywhere():
    return pl.BlockSpec(memory_space=pl.ANY)


def in_hbm(x):
    return pltpu.with_memory_space_constraint(x, pltpu.HBM)


def smem():
    return pl.BlockSpec(memory_space=pltpu.SMEM)


def call(kernel, name, outs, scratch, scalars, vectors):
    many = isinstance(outs, list)
    shapes = [jax.ShapeDtypeStruct(s, F32) for s in (outs if many else [outs])]
    return pl.pallas_call(
        kernel,
        name=name,
        out_shape=shapes if many else shapes[0],
        in_specs=[smem()] * len(scalars) + [vmem()] * len(vectors),
        out_specs=[vmem()] * len(shapes) if many else vmem(),
        scratch_shapes=[pltpu.VMEM(s, F32) for s in scratch],
        compiler_params=pltpu.CompilerParams(vmem_limit_bytes=VMEM_LIMIT),
    )(*scalars, *vectors)


def body(controls, perturbations, precision_weight, north_coef, east_coef, fine_source, fine_frac):
    count = lax.axis_size("lat")
    ranks = lax.axis_size("mem")
    members, clev, _, clon = controls.shape
    lev, band, lon = perturbations.shape[1:]
    rows, fine_lon = north_coef.shape
    part = lev // ranks

    mates = [(i, i ^ 1) for i in range(count)]
    across = [(i, (i + 1) % count if i % 2 else (i - 1) % count) for i in range(count)]
    near_chips = [(i, i ^ 2) for i in range(count)]
    far_chips = [(i, (i + 2) % count if i & 2 else (i - 2) % count) for i in range(count)]

    lon_refine = refine_matrix(clon, True)
    lev_refine = refine_matrix(clev, False)
    mix = np.einsum("vl,rt->vrtl", lev_refine, PHASES).reshape(lev * band, 3 * clev)
    lon_up = jnp.asarray(lon_refine.T, BF16)
    lon_down = jnp.asarray(lon_refine, BF16)
    mix_up = jnp.asarray(np.concatenate([mix, mix], axis=1), BF16)
    mix_down = jnp.asarray(mix.T, BF16)
    pick = np.zeros((512, 512), np.float32)
    for r in range(4):
        for q in range(128):
            pick[4 * q + r, 128 * r + q] = 1.0
    pick = jnp.asarray(pick, BF16)
    order = np.eye(part * rows).reshape(part, rows, part, rows).transpose(1, 0, 2, 3)
    order = jnp.asarray(order.reshape(part * rows, part * rows), BF16)

    own = controls.reshape(members * clev, clon)
    low_high = [lax.ppermute(own, "lat", across), lax.ppermute(own, "lat", mates)]

    flat_shape = (members * clev, clon)
    own_copy, lon_copy, mix_copy, pert, *fetched = pl.pallas_call(
        arrange_kernel,
        name="arrange",
        out_shape=[
            jax.ShapeDtypeStruct(flat_shape, F32),
            jax.ShapeDtypeStruct(lon_up.shape, BF16),
            jax.ShapeDtypeStruct(mix_up.shape, BF16),
            jax.ShapeDtypeStruct((members, lev * band, lon), BF16),
            jax.ShapeDtypeStruct((part, rows, fine_lon), BF16),
            jax.ShapeDtypeStruct((rows, fine_lon), F32),
            jax.ShapeDtypeStruct((rows, fine_lon), F32),
            jax.ShapeDtypeStruct(pick.shape, BF16),
            jax.ShapeDtypeStruct(order.shape, BF16),
        ],
        in_specs=[anywhere()] * 9,
        out_specs=[vmem()] * 9,
        scratch_shapes=[
            pltpu.VMEM((members, lev, band, lon), BF16),
            pltpu.VMEM((members, lev * band, lon), F32),
            pltpu.SemaphoreType.DMA((members + 8,)),
        ],
        compiler_params=pltpu.CompilerParams(vmem_limit_bytes=VMEM_LIMIT),
    )(
        *[in_hbm(x) for x in (own, lon_up, mix_up, perturbations)],
        *[in_hbm(x) for x in (precision_weight, north_coef, east_coef, pick, order)],
    )

    spots = 8 * PASSES + 2 * HALO + 4
    coef, own_weight, buf_a, buf_b = pl.pallas_call(
        prepare_kernel,
        name="prepare",
        out_shape=[
            jax.ShapeDtypeStruct((2 * rows, fine_lon), F32),
            jax.ShapeDtypeStruct((rows, part, fine_lon), BF16),
            jax.ShapeDtypeStruct((spots, fine_lon), F32),
            jax.ShapeDtypeStruct((spots, fine_lon), F32),
        ],
        in_specs=[smem()] * 2 + [vmem()] * 5,
        out_specs=[vmem()] * 4,
        scratch_shapes=[pltpu.VMEM((4, fine_lon), F32)],
        compiler_params=pltpu.CompilerParams(vmem_limit_bytes=VMEM_LIMIT),
    )(
        fine_source, fine_frac, *fetched,
    )
    far_b = lax.ppermute(buf_b, "lat", across)
    far_a = lax.ppermute(buf_a, "lat", mates)

    local_sum = call(
        raise_kernel, "raise", (ranks, part * band, lon),
        [(3 * members * clev, clon), (lev * band, lon)],
        [], [low_high[1], low_high[0], own_copy, lon_copy, mix_copy, pert],
    )
    parts = lax.all_to_all(local_sum, "mem", 0, 0, tiled=True)
    mine = call(total_kernel, "total", (band * part, lon), [(band * part * lon // 128, 128)], [], [parts])
    mate = lax.ppermute(mine, "lat", mates)
    pair = call(join_kernel, "join", (2 * band * part, lon), [], [], [mine, mate])
    far_pair = lax.ppermute(pair, "lat", far_chips)
    near_pair = lax.ppermute(pair, "lat", near_chips)

    n = rows + 2 * HALO
    north, east, west, weight = call(
        assemble_kernel, "assemble",
        [(n, 8, fine_lon), (n, 8, fine_lon), (n, 8, lon), (rows + 2 * PASSES, 8, fine_lon)],
        [], [], [coef, own_weight, far_a, far_b],
    )
    piece = jax.ShapeDtypeStruct((band * part, lon), F32)
    keep, send_a, send_b = pl.pallas_call(
        fine_kernel,
        name="fine",
        out_shape=[piece] * 3,
        in_specs=[anywhere()] * 4 + [vmem()] * 8,
        out_specs=[vmem()] * 3,
        scratch_shapes=[
            pltpu.VMEM((5 * band, 8, lon), F32),
            pltpu.VMEM((n, 8, fine_lon), F32),
            pltpu.VMEM((3 * band, 8, lon), F32),
            pltpu.SMEM((1, 128), F32),
            pltpu.SMEM((1, 128), F32),
            pltpu.SMEM((rows,), jnp.int32),
            pltpu.SMEM((rows,), F32),
            pltpu.SemaphoreType.DMA((4,)),
        ],
        compiler_params=pltpu.CompilerParams(vmem_limit_bytes=VMEM_LIMIT),
    )(
        fine_source, fine_frac, far_a, far_b, mine, mate, near_pair, far_pair,
        north, east, west, weight,
    )
    got_b = lax.ppermute(send_b, "lat", across)
    got_a = lax.ppermute(send_a, "lat", mates)
    copies = call(
        copies_kernel, "copies", (ranks, band * part, lon),
        [(band * part * lon // 128, 128)], [], [keep, got_a, got_b]
    )
    adjoint = lax.all_to_all(copies, "mem", 0, 0, tiled=True)
    flat = (members * clev, clon)
    result, send_a, send_b = call(
        lower_kernel, "lower", [flat, flat, flat], [(3 * members * clev, lon)],
        [], [own, pert, adjoint, mix_down, lon_down],
    )
    got_b = lax.ppermute(send_b, "lat", across)
    got_a = lax.ppermute(send_a, "lat", mates)
    return (result + got_a + got_b).reshape(controls.shape)


def solution(mesh):
    in_specs = (
        P("mem", None, "lat", None),
        P("mem", None, "lat", None),
        P(None, "lat", None),
        P("lat", None),
        P("lat", None),
        P("lat"),
        P("lat"),
    )
    out_specs = P("mem", None, "lat", None)
    return jax.shard_map(body, mesh=mesh, in_specs=in_specs, out_specs=out_specs, check_vma=False)
```

```python
import jax
import jax.numpy as jnp
import numpy as np
from jax import lax
from jax.experimental import pallas as pl
from jax.experimental.pallas import tpu as pltpu
from jax.sharding import PartitionSpec as P

PASSES = 5
REACH = 4
HALO = 2 * PASSES
VMEM_LIMIT = 24 * 2**20
F32 = jnp.float32
BF16 = jnp.bfloat16

PHASES = np.array(
    [[0.375, 0.625, 0.0], [0.125, 0.875, 0.0], [0.0, 0.875, 0.125], [0.0, 0.625, 0.375]]
)


def refine_matrix(count, periodic):
    matrix = np.zeros((4 * count, count), np.float32)
    for q in range(count):
        for r in range(4):
            for step in range(3):
                source = q + step - 1
                source = source % count if periodic else min(max(source, 0), count - 1)
                matrix[4 * q + r, source] += PHASES[r, step]
    return matrix


def split2(x):
    hi = x.astype(BF16)
    lo = (x - hi.astype(F32)).astype(BF16)
    return hi, lo


def position():
    lat = lax.axis_index("lat")
    return lat, lat % 2, lax.axis_size("lat") - 1


def dot(a, b):
    return jnp.dot(a, b, preferred_element_type=F32)


def prepare_kernel(
    source, frac, level_weight, north, east, select, order,
    coef, own_weight, buf_a, buf_b, extra,
):
    _, odd, _ = position()
    levels, rows, lon = level_weight.shape
    lane = lax.broadcasted_iota(jnp.int32, (4, 128), 1)
    tail = jnp.zeros((4, 128), F32)
    for k in range(rows):
        tail = jnp.where(lane == k, frac[k], tail)
        tail = jnp.where(lane == rows + k, source[k].astype(F32), tail)
    extra[...] = jnp.zeros(extra.shape, F32)
    extra[:, 0:128] = tail
    stacked = jnp.concatenate([north[...], east[...]], axis=0)
    hi = stacked.astype(BF16)
    rest = stacked - hi.astype(F32)
    mid = rest.astype(BF16)
    low = (rest - mid.astype(F32)).astype(BF16)
    values = dot(order[...], level_weight[...].reshape(levels * rows, lon)).astype(BF16)
    everything = jnp.concatenate([values, hi, mid, low], axis=0)
    many = levels * rows
    quarter = lon // 4
    for c in range(lon // 512):
        moved = dot(everything[:, 512 * c : 512 * c + 512], select[...])
        wpart = moved[:many]
        cpart = moved[many : many + 2 * rows] + moved[many + 2 * rows : many + 4 * rows]
        cpart = cpart + moved[many + 4 * rows :]
        for r in range(4):
            to = slice(quarter * r + 128 * c, quarter * r + 128 * c + 128)
            frm = slice(128 * r, 128 * r + 128)
            coef[:, to] = cpart[:, frm]
            own_weight[:, :, to] = wpart[:, frm].reshape(rows, levels, 128).astype(BF16)

    def fill(buf, upper):
        first = rows - PASSES if upper else 0
        for k in range(PASSES):
            buf[8 * k : 8 * k + 8, :] = own_weight[first + k].astype(F32)
        first = rows - HALO if upper else 0
        base = 8 * PASSES
        buf[base : base + HALO, :] = coef[first : first + HALO, :]
        buf[base + HALO : base + 2 * HALO, :] = coef[rows + first : rows + first + HALO, :]
        buf[base + 2 * HALO :, :] = extra[...]

    @pl.when(odd == 0)
    def _():
        fill(buf_a, True)
        fill(buf_b, False)

    @pl.when(odd == 1)
    def _():
        fill(buf_a, False)
        fill(buf_b, True)


def assemble_kernel(coef, own_weight, got_a, got_b, north, east, west, weight):
    lat, odd, _ = position()
    rows = own_weight.shape[0]
    quarter = coef.shape[1] // 4

    def put(i, nrow, erow):
        shape = (8, coef.shape[1])
        north[i] = jnp.broadcast_to(nrow, shape)
        spread = jnp.broadcast_to(erow, shape)
        east[i] = spread
        west[i] = pltpu.roll(spread[:, 3 * quarter :], 1, axis=1)

    for k in range(rows):
        put(HALO + k, coef[k : k + 1, :], coef[rows + k : rows + k + 1, :])
        weight[PASSES + k] = own_weight[k].astype(F32)

    def side(buf, start, wstart):
        base = 8 * PASSES
        for k in range(HALO):
            put(start + k, buf[base + k : base + k + 1, :], buf[base + HALO + k : base + HALO + k + 1, :])
        for k in range(PASSES):
            weight[wstart + k] = buf[8 * k : 8 * k + 8, :]

    @pl.when(odd == 0)
    def _():
        side(got_b, 0, 0)
        side(got_a, HALO + rows, PASSES + rows)

    @pl.when(odd == 1)
    def _():
        side(got_a, 0, 0)
        side(got_b, HALO + rows, PASSES + rows)

    @pl.when(lat == 0)
    def _():
        north[HALO - 1] = jnp.zeros(north.shape[1:], F32)


def arrange_kernel(
    own_all, lon_all, mix_all, stored, weight_all, north_all, east_all, select_all, order_all,
    own, lon_up, mix, pert, weight, north, east, select, order, raw, flat, sems,
):
    members, levels, band, _ = raw.shape
    small = [
        pltpu.make_async_copy(own_all, own, sems.at[members]),
        pltpu.make_async_copy(lon_all, lon_up, sems.at[members + 1]),
        pltpu.make_async_copy(mix_all, mix, sems.at[members + 2]),
    ]
    copies = [pltpu.make_async_copy(stored.at[m], raw.at[m], sems.at[m]) for m in range(members)]
    levels_here = weight_all.at[pl.ds(lax.axis_index("mem") * weight.shape[0], weight.shape[0])]
    small += [
        pltpu.make_async_copy(levels_here, weight, sems.at[members + 3]),
        pltpu.make_async_copy(north_all, north, sems.at[members + 4]),
        pltpu.make_async_copy(east_all, east, sems.at[members + 5]),
        pltpu.make_async_copy(select_all, select, sems.at[members + 6]),
        pltpu.make_async_copy(order_all, order, sems.at[members + 7]),
    ]
    for copy in copies + small:
        copy.start()
    for m in range(members):
        copies[m].wait()
        values = raw[m].astype(F32)
        for k in range(levels):
            flat[m, band * k : band * k + band, :] = values[k]
        pert[m] = flat[m].astype(BF16)
    for copy in small:
        copy.wait()


def raise_kernel(got_a, got_b, own, lon_up, mix, pert, out, x, acc):
    lat, odd, last = position()
    members = pert.shape[0]
    lev = own.shape[0] // members

    def put(step, ref):
        for m in range(members):
            at = (3 * m + step) * lev
            x[at : at + lev, :] = ref[m * lev : m * lev + lev, :]

    put(1, own)

    @pl.when(lat == 0)
    def _():
        put(0, own)

    @pl.when((lat > 0) & (odd == 0))
    def _():
        put(0, got_b)

    @pl.when(odd == 1)
    def _():
        put(0, got_a)

    @pl.when(lat == last)
    def _():
        put(2, own)

    @pl.when((lat < last) & (odd == 1))
    def _():
        put(2, got_b)

    @pl.when(odd == 0)
    def _():
        put(2, got_a)

    hi, lo = split2(x[...])
    wide = dot(hi, lon_up[...]) + dot(lo, lon_up[...])
    for m in range(members):
        hi, lo = split2(wide[3 * lev * m : 3 * lev * (m + 1), :])
        field = dot(mix[...], jnp.concatenate([hi, lo], axis=0))
        term = field * pert[m].astype(F32)
        if m == 0:
            acc[...] = term
        elif m < members - 1:
            acc[...] += term
        else:
            out[...] = (acc[...] + term).reshape(out.shape)


def total_kernel(parts, out, sums):
    count, n, lon = parts.shape
    total = parts[0]
    for k in range(1, count):
        total = total + parts[k]
    rows = n // 8
    for c in range(lon // 128):
        lanes = slice(128 * c, 128 * c + 128)
        sums[n * c : n * c + n, :] = total[:, lanes]
        for row in range(rows):
            out[8 * row : 8 * row + 8, lanes] = sums[pl.ds(n * c + row, 8, stride=rows), :]


def join_kernel(mine, mate, out):
    half = mine.shape[0]
    out[:half] = mine[...]
    out[half:] = mate[...]


def fine_kernel(
    source_all, frac_all, far_a, far_b, own, mate, near_pair, far_pair,
    north, east, west, weight, keep, send_a, send_b, mid, v, acc, extra_a, extra_b, source, frac, sems,
):
    at = 8 * PASSES + 2 * HALO
    copies = [
        pltpu.make_async_copy(far_a.at[at : at + 1, 0:128], extra_a, sems.at[0]),
        pltpu.make_async_copy(far_b.at[at : at + 1, 0:128], extra_b, sems.at[1]),
        pltpu.make_async_copy(source_all, source, sems.at[2]),
        pltpu.make_async_copy(frac_all, frac, sems.at[3]),
    ]
    for copy in copies:
        copy.start()
    lat, odd, last = position()
    lon = own.shape[1]
    rows = source.shape[0]
    n = rows + 2 * HALO
    band = own.shape[0] // 8

    def bring(slot, ref, start):
        for k in range(band):
            mid[slot * band + k] = ref[start + 8 * k : start + 8 * k + 8, :]

    half = own.shape[0]
    bring(2, own, 0)

    def gather(even, up_pair, down_pair):
        bring(0, up_pair, 0)
        bring(4, down_pair, 0)
        if even:
            bring(1, up_pair, half)
            bring(3, mate, 0)
        else:
            bring(1, mate, 0)
            bring(3, down_pair, half)

    turn = lat % 4
    for case in range(4):

        @pl.when(turn == case)
        def _(case=case):
            if case < 2:
                gather(case % 2 == 0, far_pair, near_pair)
            else:
                gather(case % 2 == 0, near_pair, far_pair)

    copies[2].wait()
    copies[3].wait()
    origin = (lat - 2) * band
    inner = list(range(HALO, HALO + rows))
    for i in inner + [i for i in range(n) if i not in inner]:
        if i == 0:
            copies[0].wait()
            copies[1].wait()
        k = i - HALO
        if k < 0:
            k += rows
            f = jnp.where(odd == 1, extra_a[0, k], extra_b[0, k])
            s = jnp.where(odd == 1, extra_a[0, rows + k], extra_b[0, rows + k]).astype(jnp.int32)
            valid = jnp.where(lat > 0, 1.0, 0.0)
        elif k >= rows:
            k -= rows
            f = jnp.where(odd == 0, extra_a[0, k], extra_b[0, k])
            s = jnp.where(odd == 0, extra_a[0, rows + k], extra_b[0, rows + k]).astype(jnp.int32)
            valid = jnp.where(lat < last, 1.0, 0.0)
        else:
            f, s, valid = frac[k], source[k], None
        s = jnp.clip(s - origin, 0, 5 * band - 2)
        below, above = 1.0 - f, f
        if valid is not None:
            below, above = below * valid, above * valid
        cur = below * mid[s] + above * mid[s + 1]
        prev = pltpu.roll(cur, 1, axis=1)
        nxt = pltpu.roll(cur, lon - 1, axis=1)
        v[i, :, 0:lon] = 0.375 * prev + 0.625 * cur
        v[i, :, lon : 2 * lon] = 0.125 * prev + 0.875 * cur
        v[i, :, 2 * lon : 3 * lon] = 0.875 * cur + 0.125 * nxt
        v[i, :, 3 * lon : 4 * lon] = 0.625 * cur + 0.375 * nxt

    inside_top = jnp.where(lat < last, 1.0, 0.0)

    def cut(r):
        return slice(r * lon, r * lon + lon)

    def sweep(first, stop, finish):
        def flux(i, here, there):
            return [north[i, :, cut(r)] * (there[r] - here[r]) for r in range(4)]

        before = [v[first - 1, :, cut(r)] for r in range(4)]
        here = [v[first, :, cut(r)] for r in range(4)]
        low = flux(first - 1, before, here)
        for i in range(first, stop):
            there = [v[i + 1, :, cut(r)] for r in range(4)]
            high = flux(i, here, there)
            if i == HALO + rows:
                low = [inside_top * x for x in low]
            right = pltpu.roll(here[0], lon - 1, axis=1)
            left = pltpu.roll(here[3], 1, axis=1)
            side = [
                east[i, :, cut(r)] * ((here[r + 1] if r < 3 else right) - here[r]) for r in range(4)
            ]
            back = [west[i] * (here[0] - left)] + side[:3]
            new = [here[r] + ((high[r] - low[r]) + (side[r] - back[r])) for r in range(4)]
            finish(i, new)
            low, here = high, there

    def store(i, new):
        for r in range(4):
            v[i, :, cut(r)] = new[r]

    def store_weighted(i, new):
        for r in range(4):
            v[i, :, cut(r)] = weight[i - PASSES, :, cut(r)] * new[r]

    acc[...] = jnp.zeros(acc.shape, F32)
    base = (lat - 1) * band

    def spread(i, o):
        k = i - HALO
        ahead = pltpu.roll(0.375 * o[0] + 0.125 * o[1], lon - 1, axis=1)
        behind = pltpu.roll(0.125 * o[2] + 0.375 * o[3], 1, axis=1)
        g = 0.625 * (o[0] + o[3]) + 0.875 * (o[1] + o[2]) + (ahead + behind)
        s = jnp.clip(source[k] - base, 0, 3 * band - 2)
        f = frac[k]
        acc[s] += (1.0 - f) * g
        acc[s + 1] += f * g

    def twice(first, stop):
        def one_pass(_, carry):
            sweep(first, stop, store)
            return carry

        lax.fori_loop(0, 2, one_pass, 0)

    twice(1, n - 1)
    twice(3, n - 3)
    sweep(PASSES, n - PASSES, store_weighted)
    twice(PASSES + 1, n - PASSES - 1)
    twice(PASSES + 3, n - PASSES - 3)
    sweep(HALO, HALO + rows, spread)
    for k in range(band):
        keep[8 * k : 8 * k + 8, :] = acc[band + k]

    def give(ref, slot):
        for k in range(band):
            ref[8 * k : 8 * k + 8, :] = acc[slot * band + k]

    @pl.when(odd == 0)
    def _():
        give(send_a, 2)
        give(send_b, 0)

    @pl.when(odd == 1)
    def _():
        give(send_a, 0)
        give(send_b, 2)


def copies_kernel(keep, got_a, got_b, out, sums):
    count, n, lon = out.shape
    rows = n // 8
    total = keep[...] + got_a[...] + got_b[...]
    for c in range(lon // 128):
        lanes = slice(128 * c, 128 * c + 128)
        for row in range(rows):
            sums[pl.ds(n * c + row, 8, stride=rows), :] = total[8 * row : 8 * row + 8, lanes]
        value = sums[n * c : n * c + n, :]
        for k in range(count):
            out[k, :, lanes] = value


def lower_kernel(controls, pert, adjoint, mix_t, lon_down, own, send_a, send_b, wide):
    lat, odd, last = position()
    members = pert.shape[0]
    lev = own.shape[0] // members
    field = adjoint[...].reshape(pert.shape[1], pert.shape[2])
    for m in range(members):
        hi, lo = split2(field * pert[m].astype(F32))
        wide[3 * lev * m : 3 * lev * (m + 1), :] = dot(mix_t[...], hi) + dot(mix_t[...], lo)
    hi, lo = split2(wide[...])
    narrow = dot(hi, lon_down[...]) + dot(lo, lon_down[...])
    at_first = jnp.where(lat == 0, 1.0, 0.0)
    at_last = jnp.where(lat == last, 1.0, 0.0)
    is_odd = jnp.where(odd == 1, 1.0, 0.0)
    for m in range(members):
        at = 3 * lev * m
        low = narrow[at : at + lev]
        mine = narrow[at + lev : at + 2 * lev]
        high = narrow[at + 2 * lev : at + 3 * lev]
        to = slice(m * lev, m * lev + lev)
        own[to, :] = controls[to, :] + mine + at_first * low + at_last * high
        low = (1.0 - at_first) * low
        high = (1.0 - at_last) * high
        send_a[to, :] = is_odd * low + (1.0 - is_odd) * high
        send_b[to, :] = is_odd * high + (1.0 - is_odd) * low


def vmem():
    return pl.BlockSpec(memory_space=pltpu.VMEM)


def anywhere():
    return pl.BlockSpec(memory_space=pl.ANY)


def in_hbm(x):
    return pltpu.with_memory_space_constraint(x, pltpu.HBM)


def smem():
    return pl.BlockSpec(memory_space=pltpu.SMEM)


def call(kernel, name, outs, scratch, scalars, vectors):
    many = isinstance(outs, list)
    shapes = [jax.ShapeDtypeStruct(s, F32) for s in (outs if many else [outs])]
    return pl.pallas_call(
        kernel,
        name=name,
        out_shape=shapes if many else shapes[0],
        in_specs=[smem()] * len(scalars) + [vmem()] * len(vectors),
        out_specs=[vmem()] * len(shapes) if many else vmem(),
        scratch_shapes=[pltpu.VMEM(s, F32) for s in scratch],
        compiler_params=pltpu.CompilerParams(vmem_limit_bytes=VMEM_LIMIT),
    )(*scalars, *vectors)


def body(controls, perturbations, precision_weight, north_coef, east_coef, fine_source, fine_frac):
    count = lax.axis_size("lat")
    ranks = lax.axis_size("mem")
    members, clev, _, clon = controls.shape
    lev, band, lon = perturbations.shape[1:]
    rows, fine_lon = north_coef.shape
    part = lev // ranks

    mates = [(i, i ^ 1) for i in range(count)]
    across = [(i, (i + 1) % count if i % 2 else (i - 1) % count) for i in range(count)]
    near_chips = [(i, i ^ 2) for i in range(count)]
    far_chips = [(i, (i + 2) % count if i & 2 else (i - 2) % count) for i in range(count)]

    lon_refine = refine_matrix(clon, True)
    lev_refine = refine_matrix(clev, False)
    mix = np.einsum("vl,rt->vrtl", lev_refine, PHASES).reshape(lev * band, 3 * clev)
    lon_up = jnp.asarray(lon_refine.T, BF16)
    lon_down = jnp.asarray(lon_refine, BF16)
    mix_up = jnp.asarray(np.concatenate([mix, mix], axis=1), BF16)
    mix_down = jnp.asarray(mix.T, BF16)
    pick = np.zeros((512, 512), np.float32)
    for r in range(4):
        for q in range(128):
            pick[4 * q + r, 128 * r + q] = 1.0
    pick = jnp.asarray(pick, BF16)
    order = np.eye(part * rows).reshape(part, rows, part, rows).transpose(1, 0, 2, 3)
    order = jnp.asarray(order.reshape(part * rows, part * rows), BF16)

    own = controls.reshape(members * clev, clon)
    low_high = [lax.ppermute(own, "lat", across), lax.ppermute(own, "lat", mates)]

    flat_shape = (members * clev, clon)
    own_copy, lon_copy, mix_copy, pert, *fetched = pl.pallas_call(
        arrange_kernel,
        name="arrange",
        out_shape=[
            jax.ShapeDtypeStruct(flat_shape, F32),
            jax.ShapeDtypeStruct(lon_up.shape, BF16),
            jax.ShapeDtypeStruct(mix_up.shape, BF16),
            jax.ShapeDtypeStruct((members, lev * band, lon), BF16),
            jax.ShapeDtypeStruct((part, rows, fine_lon), BF16),
            jax.ShapeDtypeStruct((rows, fine_lon), F32),
            jax.ShapeDtypeStruct((rows, fine_lon), F32),
            jax.ShapeDtypeStruct(pick.shape, BF16),
            jax.ShapeDtypeStruct(order.shape, BF16),
        ],
        in_specs=[anywhere()] * 9,
        out_specs=[vmem()] * 9,
        scratch_shapes=[
            pltpu.VMEM((members, lev, band, lon), BF16),
            pltpu.VMEM((members, lev * band, lon), F32),
            pltpu.SemaphoreType.DMA((members + 8,)),
        ],
        compiler_params=pltpu.CompilerParams(vmem_limit_bytes=VMEM_LIMIT),
    )(
        *[in_hbm(x) for x in (own, lon_up, mix_up, perturbations)],
        *[in_hbm(x) for x in (precision_weight, north_coef, east_coef, pick, order)],
    )

    spots = 8 * PASSES + 2 * HALO + 4
    coef, own_weight, buf_a, buf_b = pl.pallas_call(
        prepare_kernel,
        name="prepare",
        out_shape=[
            jax.ShapeDtypeStruct((2 * rows, fine_lon), F32),
            jax.ShapeDtypeStruct((rows, part, fine_lon), BF16),
            jax.ShapeDtypeStruct((spots, fine_lon), F32),
            jax.ShapeDtypeStruct((spots, fine_lon), F32),
        ],
        in_specs=[smem()] * 2 + [vmem()] * 5,
        out_specs=[vmem()] * 4,
        scratch_shapes=[pltpu.VMEM((4, fine_lon), F32)],
        compiler_params=pltpu.CompilerParams(vmem_limit_bytes=VMEM_LIMIT),
    )(
        fine_source, fine_frac, *fetched,
    )
    far_b = lax.ppermute(buf_b, "lat", across)
    far_a = lax.ppermute(buf_a, "lat", mates)

    local_sum = call(
        raise_kernel, "raise", (ranks, part * band, lon),
        [(3 * members * clev, clon), (lev * band, lon)],
        [], [low_high[1], low_high[0], own_copy, lon_copy, mix_copy, pert],
    )
    parts = lax.all_to_all(local_sum, "mem", 0, 0, tiled=True)
    mine = call(total_kernel, "total", (band * part, lon), [(band * part * lon // 128, 128)], [], [parts])
    mate = lax.ppermute(mine, "lat", mates)
    pair = call(join_kernel, "join", (2 * band * part, lon), [], [], [mine, mate])
    far_pair = lax.ppermute(pair, "lat", far_chips)
    near_pair = lax.ppermute(pair, "lat", near_chips)

    n = rows + 2 * HALO
    north, east, west, weight = call(
        assemble_kernel, "assemble",
        [(n, 8, fine_lon), (n, 8, fine_lon), (n, 8, lon), (rows + 2 * PASSES, 8, fine_lon)],
        [], [], [coef, own_weight, far_a, far_b],
    )
    piece = jax.ShapeDtypeStruct((band * part, lon), F32)
    keep, send_a, send_b = pl.pallas_call(
        fine_kernel,
        name="fine",
        out_shape=[piece] * 3,
        in_specs=[anywhere()] * 4 + [vmem()] * 8,
        out_specs=[vmem()] * 3,
        scratch_shapes=[
            pltpu.VMEM((5 * band, 8, lon), F32),
            pltpu.VMEM((n, 8, fine_lon), F32),
            pltpu.VMEM((3 * band, 8, lon), F32),
            pltpu.SMEM((1, 128), F32),
            pltpu.SMEM((1, 128), F32),
            pltpu.SMEM((rows,), jnp.int32),
            pltpu.SMEM((rows,), F32),
            pltpu.SemaphoreType.DMA((4,)),
        ],
        compiler_params=pltpu.CompilerParams(vmem_limit_bytes=VMEM_LIMIT),
    )(
        fine_source, fine_frac, far_a, far_b, mine, mate, near_pair, far_pair,
        north, east, west, weight,
    )
    got_b = lax.ppermute(send_b, "lat", across)
    got_a = lax.ppermute(send_a, "lat", mates)
    copies = call(
        copies_kernel, "copies", (ranks, band * part, lon),
        [(band * part * lon // 128, 128)], [], [keep, got_a, got_b]
    )
    adjoint = lax.all_to_all(copies, "mem", 0, 0, tiled=True)
    flat = (members * clev, clon)
    result, send_a, send_b = call(
        lower_kernel, "lower", [flat, flat, flat], [(3 * members * clev, lon)],
        [], [own, pert, adjoint, mix_down, lon_down],
    )
    got_b = lax.ppermute(send_b, "lat", across)
    got_a = lax.ppermute(send_a, "lat", mates)
    return (result + got_a + got_b).reshape(controls.shape)


def solution(mesh):
    in_specs = (
        P("mem", None, "lat", None),
        P("mem", None, "lat", None),
        P(None, "lat", None),
        P("lat", None),
        P("lat", None),
        P("lat"),
        P("lat"),
    )
    out_specs = P("mem", None, "lat", None)
    return jax.shard_map(body, mesh=mesh, in_specs=in_specs, out_specs=out_specs, check_vma=False)
```

```python
import jax
import jax.numpy as jnp
import numpy as np
from jax import lax
from jax.experimental import pallas as pl
from jax.experimental.pallas import tpu as pltpu
from jax.sharding import PartitionSpec as P

PASSES = 5
REACH = 4
HALO = 2 * PASSES
VMEM_LIMIT = 24 * 2**20
F32 = jnp.float32
BF16 = jnp.bfloat16

PHASES = np.array(
    [[0.375, 0.625, 0.0], [0.125, 0.875, 0.0], [0.0, 0.875, 0.125], [0.0, 0.625, 0.375]]
)


def refine_matrix(count, periodic):
    matrix = np.zeros((4 * count, count), np.float32)
    for q in range(count):
        for r in range(4):
            for step in range(3):
                source = q + step - 1
                source = source % count if periodic else min(max(source, 0), count - 1)
                matrix[4 * q + r, source] += PHASES[r, step]
    return matrix


def split2(x):
    hi = x.astype(BF16)
    lo = (x - hi.astype(F32)).astype(BF16)
    return hi, lo


def position():
    lat = lax.axis_index("lat")
    return lat, lat % 2, lax.axis_size("lat") - 1


def dot(a, b):
    return jnp.dot(a, b, preferred_element_type=F32)


def prepare_kernel(
    source, frac, level_weight, north, east, order,
    coef, own_weight, buf_a, buf_b, extra,
):
    _, odd, _ = position()
    levels, rows, lon = level_weight.shape
    lane = lax.broadcasted_iota(jnp.int32, (4, 128), 1)
    tail = jnp.zeros((4, 128), F32)
    for k in range(rows):
        tail = jnp.where(lane == k, frac[k], tail)
        tail = jnp.where(lane == rows + k, source[k].astype(F32), tail)
    extra[...] = jnp.zeros(extra.shape, F32)
    extra[:, 0:128] = tail
    stacked = jnp.concatenate([north[...], east[...]], axis=0)
    hi = stacked.astype(BF16)
    rest = stacked - hi.astype(F32)
    mid = rest.astype(BF16)
    low = (rest - mid.astype(F32)).astype(BF16)
    values = dot(order[...], level_weight[...].reshape(levels * rows, lon)).astype(BF16)
    everything = jnp.concatenate([values, hi, mid, low], axis=0)
    many = levels * rows
    entry = lax.broadcasted_iota(jnp.int32, (512, 512), 0)
    place = lax.broadcasted_iota(jnp.int32, (512, 512), 1)
    select = jnp.where(entry == 4 * (place & 127) + (place >> 7), 1.0, 0.0).astype(BF16)
    quarter = lon // 4
    for c in range(lon // 512):
        moved = dot(everything[:, 512 * c : 512 * c + 512], select)
        wpart = moved[:many]
        cpart = moved[many : many + 2 * rows] + moved[many + 2 * rows : many + 4 * rows]
        cpart = cpart + moved[many + 4 * rows :]
        for r in range(4):
            to = slice(quarter * r + 128 * c, quarter * r + 128 * c + 128)
            frm = slice(128 * r, 128 * r + 128)
            coef[:, to] = cpart[:, frm]
            own_weight[:, :, to] = wpart[:, frm].reshape(rows, levels, 128).astype(BF16)

    def fill(buf, upper):
        first = rows - PASSES if upper else 0
        for k in range(PASSES):
            buf[8 * k : 8 * k + 8, :] = own_weight[first + k].astype(F32)
        first = rows - HALO if upper else 0
        base = 8 * PASSES
        buf[base : base + HALO, :] = coef[first : first + HALO, :]
        buf[base + HALO : base + 2 * HALO, :] = coef[rows + first : rows + first + HALO, :]
        buf[base + 2 * HALO :, :] = extra[...]

    @pl.when(odd == 0)
    def _():
        fill(buf_a, True)
        fill(buf_b, False)

    @pl.when(odd == 1)
    def _():
        fill(buf_a, False)
        fill(buf_b, True)


def assemble_kernel(coef, own_weight, got_a, got_b, north, east, west, weight):
    lat, odd, _ = position()
    rows = own_weight.shape[0]
    quarter = coef.shape[1] // 4

    def put(i, nrow, erow):
        shape = (8, coef.shape[1])
        north[i] = jnp.broadcast_to(nrow, shape)
        spread = jnp.broadcast_to(erow, shape)
        east[i] = spread
        west[i] = pltpu.roll(spread[:, 3 * quarter :], 1, axis=1)

    for k in range(rows):
        put(HALO + k, coef[k : k + 1, :], coef[rows + k : rows + k + 1, :])
        weight[PASSES + k] = own_weight[k].astype(F32)

    def side(buf, start, wstart):
        base = 8 * PASSES
        for k in range(HALO):
            put(start + k, buf[base + k : base + k + 1, :], buf[base + HALO + k : base + HALO + k + 1, :])
        for k in range(PASSES):
            weight[wstart + k] = buf[8 * k : 8 * k + 8, :]

    @pl.when(odd == 0)
    def _():
        side(got_b, 0, 0)
        side(got_a, HALO + rows, PASSES + rows)

    @pl.when(odd == 1)
    def _():
        side(got_a, 0, 0)
        side(got_b, HALO + rows, PASSES + rows)

    @pl.when(lat == 0)
    def _():
        north[HALO - 1] = jnp.zeros(north.shape[1:], F32)


def arrange_kernel(
    own_all, lon_all, mix_all, stored, weight_all, north_all, east_all, order_all,
    own, lon_up, mix, pert, weight, north, east, order, raw, flat, sems,
):
    members, levels, band, _ = raw.shape
    small = [
        pltpu.make_async_copy(own_all, own, sems.at[members]),
        pltpu.make_async_copy(lon_all, lon_up, sems.at[members + 1]),
        pltpu.make_async_copy(mix_all, mix, sems.at[members + 2]),
    ]
    copies = [pltpu.make_async_copy(stored.at[m], raw.at[m], sems.at[m]) for m in range(members)]
    levels_here = weight_all.at[pl.ds(lax.axis_index("mem") * weight.shape[0], weight.shape[0])]
    small += [
        pltpu.make_async_copy(levels_here, weight, sems.at[members + 3]),
        pltpu.make_async_copy(north_all, north, sems.at[members + 4]),
        pltpu.make_async_copy(east_all, east, sems.at[members + 5]),
        pltpu.make_async_copy(order_all, order, sems.at[members + 6]),
    ]
    for copy in copies + small:
        copy.start()
    for m in range(members):
        copies[m].wait()
        values = raw[m].astype(F32)
        for k in range(levels):
            flat[m, band * k : band * k + band, :] = values[k]
        pert[m] = flat[m].astype(BF16)
    for copy in small:
        copy.wait()


def raise_kernel(got_a, got_b, own, lon_up, mix, pert, out, x, acc):
    lat, odd, last = position()
    members = pert.shape[0]
    lev = own.shape[0] // members

    def put(step, ref):
        for m in range(members):
            at = (3 * m + step) * lev
            x[at : at + lev, :] = ref[m * lev : m * lev + lev, :]

    put(1, own)

    @pl.when(lat == 0)
    def _():
        put(0, own)

    @pl.when((lat > 0) & (odd == 0))
    def _():
        put(0, got_b)

    @pl.when(odd == 1)
    def _():
        put(0, got_a)

    @pl.when(lat == last)
    def _():
        put(2, own)

    @pl.when((lat < last) & (odd == 1))
    def _():
        put(2, got_b)

    @pl.when(odd == 0)
    def _():
        put(2, got_a)

    hi, lo = split2(x[...])
    wide = dot(hi, lon_up[...]) + dot(lo, lon_up[...])
    for m in range(members):
        hi, lo = split2(wide[3 * lev * m : 3 * lev * (m + 1), :])
        field = dot(mix[...], jnp.concatenate([hi, lo], axis=0))
        term = field * pert[m].astype(F32)
        if m == 0:
            acc[...] = term
        elif m < members - 1:
            acc[...] += term
        else:
            out[...] = (acc[...] + term).reshape(out.shape)


def total_kernel(parts, out, sums):
    count, n, lon = parts.shape
    total = parts[0]
    for k in range(1, count):
        total = total + parts[k]
    rows = n // 8
    for c in range(lon // 128):
        lanes = slice(128 * c, 128 * c + 128)
        sums[n * c : n * c + n, :] = total[:, lanes]
        for row in range(rows):
            out[8 * row : 8 * row + 8, lanes] = sums[pl.ds(n * c + row, 8, stride=rows), :]


def join_kernel(mine, mate, out):
    half = mine.shape[0]
    out[:half] = mine[...]
    out[half:] = mate[...]


def fine_kernel(
    source_all, frac_all, far_a, far_b, own, mate, near_pair, far_pair,
    north, east, west, weight, keep, send_a, send_b, mid, v, acc, extra_a, extra_b, source, frac, sems,
):
    at = 8 * PASSES + 2 * HALO
    copies = [
        pltpu.make_async_copy(far_a.at[at : at + 1, 0:128], extra_a, sems.at[0]),
        pltpu.make_async_copy(far_b.at[at : at + 1, 0:128], extra_b, sems.at[1]),
        pltpu.make_async_copy(source_all, source, sems.at[2]),
        pltpu.make_async_copy(frac_all, frac, sems.at[3]),
    ]
    for copy in copies:
        copy.start()
    lat, odd, last = position()
    lon = own.shape[1]
    rows = source.shape[0]
    n = rows + 2 * HALO
    band = own.shape[0] // 8

    def bring(slot, ref, start):
        for k in range(band):
            mid[slot * band + k] = ref[start + 8 * k : start + 8 * k + 8, :]

    half = own.shape[0]
    bring(2, own, 0)

    def gather(even, up_pair, down_pair):
        bring(0, up_pair, 0)
        bring(4, down_pair, 0)
        if even:
            bring(1, up_pair, half)
            bring(3, mate, 0)
        else:
            bring(1, mate, 0)
            bring(3, down_pair, half)

    turn = lat % 4
    for case in range(4):

        @pl.when(turn == case)
        def _(case=case):
            if case < 2:
                gather(case % 2 == 0, far_pair, near_pair)
            else:
                gather(case % 2 == 0, near_pair, far_pair)

    copies[2].wait()
    copies[3].wait()
    origin = (lat - 2) * band
    inner = list(range(HALO, HALO + rows))
    for i in inner + [i for i in range(n) if i not in inner]:
        if i == 0:
            copies[0].wait()
            copies[1].wait()
        k = i - HALO
        if k < 0:
            k += rows
            f = jnp.where(odd == 1, extra_a[0, k], extra_b[0, k])
            s = jnp.where(odd == 1, extra_a[0, rows + k], extra_b[0, rows + k]).astype(jnp.int32)
            valid = jnp.where(lat > 0, 1.0, 0.0)
        elif k >= rows:
            k -= rows
            f = jnp.where(odd == 0, extra_a[0, k], extra_b[0, k])
            s = jnp.where(odd == 0, extra_a[0, rows + k], extra_b[0, rows + k]).astype(jnp.int32)
            valid = jnp.where(lat < last, 1.0, 0.0)
        else:
            f, s, valid = frac[k], source[k], None
        s = jnp.clip(s - origin, 0, 5 * band - 2)
        below, above = 1.0 - f, f
        if valid is not None:
            below, above = below * valid, above * valid
        cur = below * mid[s] + above * mid[s + 1]
        prev = pltpu.roll(cur, 1, axis=1)
        nxt = pltpu.roll(cur, lon - 1, axis=1)
        v[i, :, 0:lon] = 0.375 * prev + 0.625 * cur
        v[i, :, lon : 2 * lon] = 0.125 * prev + 0.875 * cur
        v[i, :, 2 * lon : 3 * lon] = 0.875 * cur + 0.125 * nxt
        v[i, :, 3 * lon : 4 * lon] = 0.625 * cur + 0.375 * nxt

    inside_top = jnp.where(lat < last, 1.0, 0.0)

    def cut(r):
        return slice(r * lon, r * lon + lon)

    def sweep(first, stop, finish):
        def flux(i, here, there):
            return [north[i, :, cut(r)] * (there[r] - here[r]) for r in range(4)]

        before = [v[first - 1, :, cut(r)] for r in range(4)]
        here = [v[first, :, cut(r)] for r in range(4)]
        low = flux(first - 1, before, here)
        for i in range(first, stop):
            there = [v[i + 1, :, cut(r)] for r in range(4)]
            high = flux(i, here, there)
            if i == HALO + rows:
                low = [inside_top * x for x in low]
            right = pltpu.roll(here[0], lon - 1, axis=1)
            left = pltpu.roll(here[3], 1, axis=1)
            side = [
                east[i, :, cut(r)] * ((here[r + 1] if r < 3 else right) - here[r]) for r in range(4)
            ]
            back = [west[i] * (here[0] - left)] + side[:3]
            new = [here[r] + ((high[r] - low[r]) + (side[r] - back[r])) for r in range(4)]
            finish(i, new)
            low, here = high, there

    def store(i, new):
        for r in range(4):
            v[i, :, cut(r)] = new[r]

    def store_weighted(i, new):
        for r in range(4):
            v[i, :, cut(r)] = weight[i - PASSES, :, cut(r)] * new[r]

    acc[...] = jnp.zeros(acc.shape, F32)
    base = (lat - 1) * band

    def spread(i, o):
        k = i - HALO
        ahead = pltpu.roll(0.375 * o[0] + 0.125 * o[1], lon - 1, axis=1)
        behind = pltpu.roll(0.125 * o[2] + 0.375 * o[3], 1, axis=1)
        g = 0.625 * (o[0] + o[3]) + 0.875 * (o[1] + o[2]) + (ahead + behind)
        s = jnp.clip(source[k] - base, 0, 3 * band - 2)
        f = frac[k]
        acc[s] += (1.0 - f) * g
        acc[s + 1] += f * g

    def twice(first, stop):
        def one_pass(_, carry):
            sweep(first, stop, store)
            return carry

        lax.fori_loop(0, 2, one_pass, 0)

    twice(1, n - 1)
    twice(3, n - 3)
    sweep(PASSES, n - PASSES, store_weighted)
    twice(PASSES + 1, n - PASSES - 1)
    twice(PASSES + 3, n - PASSES - 3)
    sweep(HALO, HALO + rows, spread)
    for k in range(band):
        keep[8 * k : 8 * k + 8, :] = acc[band + k]

    def give(ref, slot):
        for k in range(band):
            ref[8 * k : 8 * k + 8, :] = acc[slot * band + k]

    @pl.when(odd == 0)
    def _():
        give(send_a, 2)
        give(send_b, 0)

    @pl.when(odd == 1)
    def _():
        give(send_a, 0)
        give(send_b, 2)


def copies_kernel(keep, got_a, got_b, out, sums):
    count, n, lon = out.shape
    rows = n // 8
    total = keep[...] + got_a[...] + got_b[...]
    for c in range(lon // 128):
        lanes = slice(128 * c, 128 * c + 128)
        for row in range(rows):
            sums[pl.ds(n * c + row, 8, stride=rows), :] = total[8 * row : 8 * row + 8, lanes]
        value = sums[n * c : n * c + n, :]
        for k in range(count):
            out[k, :, lanes] = value


def lower_kernel(controls, pert, adjoint, mix_t, lon_down, own, send_a, send_b, wide):
    lat, odd, last = position()
    members = pert.shape[0]
    lev = own.shape[0] // members
    field = adjoint[...].reshape(pert.shape[1], pert.shape[2])
    for m in range(members):
        hi, lo = split2(field * pert[m].astype(F32))
        wide[3 * lev * m : 3 * lev * (m + 1), :] = dot(mix_t[...], hi) + dot(mix_t[...], lo)
    hi, lo = split2(wide[...])
    narrow = dot(hi, lon_down[...]) + dot(lo, lon_down[...])
    at_first = jnp.where(lat == 0, 1.0, 0.0)
    at_last = jnp.where(lat == last, 1.0, 0.0)
    is_odd = jnp.where(odd == 1, 1.0, 0.0)
    for m in range(members):
        at = 3 * lev * m
        low = narrow[at : at + lev]
        mine = narrow[at + lev : at + 2 * lev]
        high = narrow[at + 2 * lev : at + 3 * lev]
        to = slice(m * lev, m * lev + lev)
        own[to, :] = controls[to, :] + mine + at_first * low + at_last * high
        low = (1.0 - at_first) * low
        high = (1.0 - at_last) * high
        send_a[to, :] = is_odd * low + (1.0 - is_odd) * high
        send_b[to, :] = is_odd * high + (1.0 - is_odd) * low


def vmem():
    return pl.BlockSpec(memory_space=pltpu.VMEM)


def anywhere():
    return pl.BlockSpec(memory_space=pl.ANY)


def in_hbm(x):
    return pltpu.with_memory_space_constraint(x, pltpu.HBM)


def smem():
    return pl.BlockSpec(memory_space=pltpu.SMEM)


def call(kernel, name, outs, scratch, scalars, vectors):
    many = isinstance(outs, list)
    shapes = [jax.ShapeDtypeStruct(s, F32) for s in (outs if many else [outs])]
    return pl.pallas_call(
        kernel,
        name=name,
        out_shape=shapes if many else shapes[0],
        in_specs=[smem()] * len(scalars) + [vmem()] * len(vectors),
        out_specs=[vmem()] * len(shapes) if many else vmem(),
        scratch_shapes=[pltpu.VMEM(s, F32) for s in scratch],
        compiler_params=pltpu.CompilerParams(vmem_limit_bytes=VMEM_LIMIT),
    )(*scalars, *vectors)


def body(controls, perturbations, precision_weight, north_coef, east_coef, fine_source, fine_frac):
    count = lax.axis_size("lat")
    ranks = lax.axis_size("mem")
    members, clev, _, clon = controls.shape
    lev, band, lon = perturbations.shape[1:]
    rows, fine_lon = north_coef.shape
    part = lev // ranks

    mates = [(i, i ^ 1) for i in range(count)]
    across = [(i, (i + 1) % count if i % 2 else (i - 1) % count) for i in range(count)]
    near_chips = [(i, i ^ 2) for i in range(count)]
    far_chips = [(i, (i + 2) % count if i & 2 else (i - 2) % count) for i in range(count)]

    lon_refine = refine_matrix(clon, True)
    lev_refine = refine_matrix(clev, False)
    mix = np.einsum("vl,rt->vrtl", lev_refine, PHASES).reshape(lev * band, 3 * clev)
    lon_up = jnp.asarray(lon_refine.T, BF16)
    lon_down = jnp.asarray(lon_refine, BF16)
    mix_up = jnp.asarray(np.concatenate([mix, mix], axis=1), BF16)
    mix_down = jnp.asarray(mix.T, BF16)
    order = np.eye(part * rows).reshape(part, rows, part, rows).transpose(1, 0, 2, 3)
    order = jnp.asarray(order.reshape(part * rows, part * rows), BF16)

    own = controls.reshape(members * clev, clon)
    low_high = [lax.ppermute(own, "lat", across), lax.ppermute(own, "lat", mates)]

    flat_shape = (members * clev, clon)
    own_copy, lon_copy, mix_copy, pert, *fetched = pl.pallas_call(
        arrange_kernel,
        name="arrange",
        out_shape=[
            jax.ShapeDtypeStruct(flat_shape, F32),
            jax.ShapeDtypeStruct(lon_up.shape, BF16),
            jax.ShapeDtypeStruct(mix_up.shape, BF16),
            jax.ShapeDtypeStruct((members, lev * band, lon), BF16),
            jax.ShapeDtypeStruct((part, rows, fine_lon), BF16),
            jax.ShapeDtypeStruct((rows, fine_lon), F32),
            jax.ShapeDtypeStruct((rows, fine_lon), F32),
            jax.ShapeDtypeStruct(order.shape, BF16),
        ],
        in_specs=[anywhere()] * 8,
        out_specs=[vmem()] * 8,
        scratch_shapes=[
            pltpu.VMEM((members, lev, band, lon), BF16),
            pltpu.VMEM((members, lev * band, lon), F32),
            pltpu.SemaphoreType.DMA((members + 7,)),
        ],
        compiler_params=pltpu.CompilerParams(vmem_limit_bytes=VMEM_LIMIT),
    )(
        *[in_hbm(x) for x in (own, lon_up, mix_up, perturbations)],
        *[in_hbm(x) for x in (precision_weight, north_coef, east_coef, order)],
    )

    spots = 8 * PASSES + 2 * HALO + 4
    coef, own_weight, buf_a, buf_b = pl.pallas_call(
        prepare_kernel,
        name="prepare",
        out_shape=[
            jax.ShapeDtypeStruct((2 * rows, fine_lon), F32),
            jax.ShapeDtypeStruct((rows, part, fine_lon), BF16),
            jax.ShapeDtypeStruct((spots, fine_lon), F32),
            jax.ShapeDtypeStruct((spots, fine_lon), F32),
        ],
        in_specs=[smem()] * 2 + [vmem()] * 4,
        out_specs=[vmem()] * 4,
        scratch_shapes=[pltpu.VMEM((4, fine_lon), F32)],
        compiler_params=pltpu.CompilerParams(vmem_limit_bytes=VMEM_LIMIT),
    )(
        fine_source, fine_frac, *fetched,
    )
    far_b = lax.ppermute(buf_b, "lat", across)
    far_a = lax.ppermute(buf_a, "lat", mates)

    local_sum = call(
        raise_kernel, "raise", (ranks, part * band, lon),
        [(3 * members * clev, clon), (lev * band, lon)],
        [], [low_high[1], low_high[0], own_copy, lon_copy, mix_copy, pert],
    )
    parts = lax.all_to_all(local_sum, "mem", 0, 0, tiled=True)
    mine = call(total_kernel, "total", (band * part, lon), [(band * part * lon // 128, 128)], [], [parts])
    mate = lax.ppermute(mine, "lat", mates)
    pair = call(join_kernel, "join", (2 * band * part, lon), [], [], [mine, mate])
    far_pair = lax.ppermute(pair, "lat", far_chips)
    near_pair = lax.ppermute(pair, "lat", near_chips)

    n = rows + 2 * HALO
    north, east, west, weight = call(
        assemble_kernel, "assemble",
        [(n, 8, fine_lon), (n, 8, fine_lon), (n, 8, lon), (rows + 2 * PASSES, 8, fine_lon)],
        [], [], [coef, own_weight, far_a, far_b],
    )
    piece = jax.ShapeDtypeStruct((band * part, lon), F32)
    keep, send_a, send_b = pl.pallas_call(
        fine_kernel,
        name="fine",
        out_shape=[piece] * 3,
        in_specs=[anywhere()] * 4 + [vmem()] * 8,
        out_specs=[vmem()] * 3,
        scratch_shapes=[
            pltpu.VMEM((5 * band, 8, lon), F32),
            pltpu.VMEM((n, 8, fine_lon), F32),
            pltpu.VMEM((3 * band, 8, lon), F32),
            pltpu.SMEM((1, 128), F32),
            pltpu.SMEM((1, 128), F32),
            pltpu.SMEM((rows,), jnp.int32),
            pltpu.SMEM((rows,), F32),
            pltpu.SemaphoreType.DMA((4,)),
        ],
        compiler_params=pltpu.CompilerParams(vmem_limit_bytes=VMEM_LIMIT),
    )(
        fine_source, fine_frac, far_a, far_b, mine, mate, near_pair, far_pair,
        north, east, west, weight,
    )
    got_b = lax.ppermute(send_b, "lat", across)
    got_a = lax.ppermute(send_a, "lat", mates)
    copies = call(
        copies_kernel, "copies", (ranks, band * part, lon),
        [(band * part * lon // 128, 128)], [], [keep, got_a, got_b]
    )
    adjoint = lax.all_to_all(copies, "mem", 0, 0, tiled=True)
    flat = (members * clev, clon)
    result, send_a, send_b = call(
        lower_kernel, "lower", [flat, flat, flat], [(3 * members * clev, lon)],
        [], [own, pert, adjoint, mix_down, lon_down],
    )
    got_b = lax.ppermute(send_b, "lat", across)
    got_a = lax.ppermute(send_a, "lat", mates)
    return (result + got_a + got_b).reshape(controls.shape)


def solution(mesh):
    in_specs = (
        P("mem", None, "lat", None),
        P("mem", None, "lat", None),
        P(None, "lat", None),
        P("lat", None),
        P("lat", None),
        P("lat"),
        P("lat"),
    )
    out_specs = P("mem", None, "lat", None)
    return jax.shard_map(body, mesh=mesh, in_specs=in_specs, out_specs=out_specs, check_vma=False)
```
